32 devices in a mesh: frame: 8 (over z, x), head: 4 (over y, core).
Axes of the slice: x: 2, y: 2, z: 4, core: 2. Of those that a mesh axis runs over, the one named last changes fastest.
Arguments:
- queries: bfloat16 [4096, 1024], P('frame', 'head'), may hold values from -6 to 6
- keys: bfloat16 [4096, 1024], P('frame', 'head'), may hold values from -6 to 6
- values: bfloat16 [4096, 1024], P('frame', 'head'), may hold values from -6 to 6
- band_width: int32 [8, 8], replicated, may hold values from 1 to 4, as said below
- band_offset: int32 [8, 8, 4], replicated, may hold values from 0 to 3
- out_weight: bfloat16 [1024, 1536], P('head'), may hold values from -0.1875 to 0.1875
Outputs:
- projected: bfloat16 [4096, 1536], P(('frame', 'head'))
The draws below stay inside these ranges and needn't reach their ends.
Inputs may be any that keep to these rules, and one draw needn't show every extreme that they name: `band_width`: for distances 0 and 1 the widths lie in (2, 4], for 2 and 3 in (1, 2], for 4 to 7 in [1, 1]; each of these upper ends is reached by some frame.
All inputs are finite; a program needn't handle non-finite values.
Results may differ from the reference program's by a relative error of at most 0.015.
Values may be sent and summed in bfloat16 or wider, within the bound.
No kernel may reach another device: no remote copies, remote signals or barrier semaphores. Data moves between devices by JAX's collectives and lax.ppermute only.
A program may use at most 64 MiB of HBM per device.

```python
import math
import jax
import jax.numpy as jnp
from jax import lax

D = 1536
HEADS = 8
HEAD = 128
TF = 512
BLK = 128
RADIUS = 7
FRAMES = 8
NB = 4
TOKENS = 4096


def paired_draw(key):
    keys_raw = jnp.clip(jax.random.normal(jax.random.fold_in(key, 11), (TOKENS, HEADS * HEAD), jnp.float32), -6.0, 6.0)
    query_raw = jnp.clip(jax.random.normal(jax.random.fold_in(key, 12), (TOKENS, HEADS * HEAD), jnp.float32), -6.0, 6.0)
    return (query_raw, keys_raw)


def draw_queries(key, part):
    query_raw, keys_raw = paired_draw(key)
    return query_raw.astype(jnp.bfloat16)


def draw_keys(key, part):
    query_raw, keys_raw = paired_draw(key)
    return keys_raw.astype(jnp.bfloat16)


def draw_band_width(key, part):
    column = jnp.arange(RADIUS + 1)
    upper = jnp.where(column <= 1, NB, jnp.where(column <= 3, NB // 2, NB // 4))
    lower = jnp.where(column <= 1, NB // 2 + 1, jnp.where(column <= 3, NB // 4 + 1, 1))
    raw = jax.random.randint(jax.random.fold_in(key, 21), (FRAMES, RADIUS + 1), 0, 1 << 20)
    widths = lower[None, :] + raw % (upper - lower + 1)[None, :]
    chosen = jax.random.randint(jax.random.fold_in(key, 22), (), 0, FRAMES)
    widths = jnp.where(jnp.arange(FRAMES)[:, None] == chosen, upper[None, :], widths)
    return widths.astype(jnp.int32)


def draw_band_offset(key, part):
    return jax.random.randint(jax.random.fold_in(key, 31), (FRAMES, RADIUS + 1, NB), 0, NB).astype(jnp.int32)


def levels(own_key, shape, cuts, smallest, top_value):
    loudness = 1.0
    for position, blocks in cuts:
        heights = jax.random.uniform(jax.random.fold_in(jax.random.fold_in(own_key, 6), position), (blocks,), jnp.float32, smallest / len(cuts), top_value / len(cuts))
        loudness = loudness * jnp.repeat(jnp.exp(heights), shape[position] // blocks).reshape((-1,) + (1,) * (len(shape) - 1 - position))
    return loudness


def bell_draw(rng, shape, scale, bound, split=(), kind=jnp.bfloat16):
    array = jax.random.normal(rng, shape, jnp.float32) * scale
    if len(split) > 0:
        array = levels(rng, shape, split, -0.22, 0.18) * array
    return jnp.clip(array, min=-bound, max=bound).astype(kind)


def setup_inputs(seed: int = 0) -> dict:
    splits = jax.random.split(jax.random.key(seed), 7)
    return {
        "queries": draw_queries(jax.random.fold_in(splits[6], 71), 0),
        "keys": draw_keys(jax.random.fold_in(splits[6], 71), 0),
        "values": bell_draw(splits[2], (TOKENS, HEADS * HEAD), 1.0, 6.0, ((0, 8), (1, 4))),
        "band_width": draw_band_width(jax.random.fold_in(splits[6], 71), 0),
        "band_offset": draw_band_offset(jax.random.fold_in(splits[6], 71), 0),
        "out_weight": bell_draw(splits[5], (HEADS * HEAD, D), (HEADS * HEAD) ** -0.5, 0.1875, ((0, 4),)),
    }


def block_mask(this_frame, key_frame, frames, band_width, band_offset, block_count):
    distance = jnp.abs(key_frame - this_frame)
    present = (key_frame >= 0) & (key_frame < frames) & (distance <= RADIUS)
    reach = jnp.minimum(distance, RADIUS)
    band_span = band_width[this_frame, reach]
    offsets = band_offset[this_frame, reach]
    query_block = lax.broadcasted_iota(jnp.int32, (block_count, block_count), 0)
    key_block = lax.broadcasted_iota(jnp.int32, (block_count, block_count), 1)
    inside = jnp.mod(key_block - offsets[:, None], block_count) < band_span
    diagonal = (reach == 0) & (query_block == key_block)
    return present & (inside | diagonal)

def reference(queries, keys, values, band_width, band_offset, out_weight):
    score_scale = 1.0 / math.sqrt(HEAD)

    def attend_pair(pair):
        this_frame = (pair // HEADS).astype(jnp.int32)
        head_index = (pair % HEADS).astype(jnp.int32)
        column = (head_index * HEAD).astype(jnp.int32)
        query_rows = lax.dynamic_slice(queries, ((this_frame * TF).astype(jnp.int32), column), (TF, HEAD))
        key_list = []
        value_list = []
        mask_list = []
        for shift_step in range(-RADIUS, RADIUS + 1):
            key_frame = this_frame + shift_step
            clipped = jnp.clip(key_frame, 0, FRAMES - 1).astype(jnp.int32)
            start_row = (clipped * TF).astype(jnp.int32)
            key_list.append(lax.dynamic_slice(keys, (start_row, column), (TF, HEAD)))
            value_list.append(lax.dynamic_slice(values, (start_row, column), (TF, HEAD)))
            blocks = block_mask(this_frame, key_frame, FRAMES, band_width, band_offset, NB)
            mask_list.append(jnp.repeat(jnp.repeat(blocks, BLK, axis=0), BLK, axis=1))
        key_all = jnp.concatenate(key_list, axis=0)
        value_all = jnp.concatenate(value_list, axis=0)
        mask_all = jnp.concatenate(mask_list, axis=1)
        scores = jnp.dot(query_rows, key_all.T, preferred_element_type=jnp.float32) * score_scale
        scores = jnp.where(mask_all, scores, -1e+30)
        peak = lax.optimization_barrier(jnp.max(scores, axis=1, keepdims=True))
        weights = jnp.where(mask_all, jnp.exp(scores - peak), 0.0)
        totals = lax.optimization_barrier(jnp.sum(weights, axis=1, keepdims=True))
        mixed = jnp.dot(weights.astype(jnp.bfloat16), value_all, preferred_element_type=jnp.float32)
        return mixed / totals
    pairs = jnp.arange(FRAMES * HEADS, dtype=jnp.int32)
    heads_out = lax.map(attend_pair, pairs)
    attended = heads_out.reshape(FRAMES, HEADS, TF, HEAD).transpose(0, 2, 1, 3)
    attended = attended.reshape(TOKENS, HEADS * HEAD).astype(jnp.bfloat16)
    return jnp.dot(attended, out_weight, preferred_element_type=jnp.float32).astype(jnp.bfloat16)
```

```python
import functools
import math

import jax
import jax.numpy as jnp
from jax import lax
from jax.experimental import pallas as pl
from jax.experimental.pallas import tpu as pltpu
from jax.sharding import PartitionSpec as P

HEAD = 128
BLK = 128
RADIUS = 7
MAX_WIDTH = (4, 4, 2, 2, 1, 1, 1, 1)
MASKED = -1e30
EXPONENT = math.log2(math.e) / math.sqrt(HEAD)

VMEM = pl.BlockSpec(memory_space=pltpu.VMEM)
SMEM = pl.BlockSpec(memory_space=pltpu.SMEM)
HBM = pl.BlockSpec(memory_space=pltpu.HBM)


def in_vmem(value):
    return pltpu.with_memory_space_constraint(value, pltpu.VMEM)


def params():
    return pltpu.CompilerParams(vmem_limit_bytes=32 << 20)


def split_kernel(group, q_ref, k_ref, v_ref, *refs):
    outs, sem = refs[:-1], refs[-1]
    width = outs[0].shape[1] // 2
    place = lax.rem(lax.axis_index("frame"), group)
    copies = []
    for part in range(group):
        column = (place if part == 0 else 1 - place) * width
        columns = pl.ds(pl.multiple_of(column, HEAD), width)
        pair, rows = outs[2 * part], outs[2 * part + 1]
        for source, target in (
            (k_ref, pair.at[:, :width]),
            (v_ref, pair.at[:, width:]),
            (q_ref, rows),
        ):
            copies.append(
                pltpu.make_async_copy(source.at[:, columns], target, sem.at[len(copies)])
            )
    for copy in copies:
        copy.start()
    for copy in copies:
        copy.wait()


def split(queries, keys, values, group):
    tokens, columns = queries.shape
    width = columns // group
    pair = pltpu.VMEM((tokens, 2 * width), queries.dtype)
    rows = pltpu.VMEM((tokens, width), queries.dtype)
    return pl.pallas_call(
        functools.partial(split_kernel, group),
        out_shape=[pair, rows] * group,
        in_specs=[HBM] * 3,
        out_specs=[VMEM] * (2 * group),
        scratch_shapes=[pltpu.SemaphoreType.DMA((3 * group,))],
        compiler_params=params(),
        name="split",
    )(queries, keys, values)


def frame_of(unit, place, group, member):
    return unit * group + (place if member == 0 else group - 1 - place)


def update(b, rows, query, key_slots, value_slots, oks, m_ref, acc_ref, head, first):
    scores = lax.dot_general(
        query, key_slots, (((1,), (1,)), ((), ())), preferred_element_type=jnp.float32
    )
    pieces = [scores[:, BLK * j : BLK * (j + 1)] for j in range(len(oks))]
    pieces = [s if ok is None else jnp.where(ok, s, MASKED) for s, ok in zip(pieces, oks)]
    tallest = functools.reduce(jnp.maximum, pieces)
    tallest = jnp.max(tallest, axis=1, keepdims=True)
    if first:
        peak = jnp.broadcast_to(tallest, (BLK, BLK))
    else:
        before = m_ref[head, rows, :]
        peak = jnp.maximum(before, tallest)
    weights = [jnp.exp2((s - peak) * EXPONENT).astype(jnp.bfloat16) for s in pieces]
    weights = jnp.concatenate(weights, axis=1)
    added = jnp.dot(weights, value_slots, preferred_element_type=jnp.float32)
    if not first:
        rescale = jnp.exp2((before - peak) * EXPONENT)
        rescale = jnp.concatenate([rescale, rescale], axis=1)
        added = acc_ref[head, rows, :] * rescale + added
    acc_ref[head, rows, :] = added
    m_ref[head, rows, :] = peak


def attend_kernel(cfg, width_ref, offset_ref, *refs):
    group, heads, shifts, units, begins, ends = cfg
    q_refs, refs = refs[:group], refs[group:]
    chunks = [refs[group * i : group * (i + 1)] for i in range(len(shifts))]
    refs = refs[group * len(shifts) :]
    if not begins:
        refs = refs[2:]
    if ends:
        out_ref, m_ref, acc_ref = refs
    else:
        m_ref, acc_ref = refs
    tokens = q_refs[0].shape[0]
    blocks = tokens // BLK
    width = heads * HEAD
    me = lax.axis_index("frame")
    unit, place = me // group, lax.rem(me, group)
    ones = jnp.ones((BLK, HEAD), jnp.bfloat16)

    def pair_slots(b, qf, kf, far, member, refs):
        distance = jnp.abs(qf - kf)
        present = distance <= RADIUS
        reach = jnp.minimum(distance, RADIUS)
        span = width_ref[qf, reach]
        start = offset_ref[qf, reach, b]
        most = min(MAX_WIDTH[min(far, RADIUS)], blocks)
        found = []
        for j in range(most):
            if most == blocks:
                inside = lax.rem(j - start + blocks, blocks) < span
                if far == 0:
                    inside = inside | ((distance == 0) & (b == j))
                found.append((refs, j, present & inside))
            else:
                inside = None if most == 1 and far * 1 <= RADIUS - 2 * (group - 1) else present & (j < span)
                found.append((refs, lax.rem(start + j, blocks), inside))
        return found

    def gather(found, head, column):
        parts = []
        for ref, block, _ in found:
            if isinstance(block, int):
                at = pl.ds(block * BLK, BLK)
            else:
                at = pl.ds(pl.multiple_of(block * BLK, BLK), BLK)
            parts.append(ref[at, column + head * HEAD : column + (head + 1) * HEAD])
        return parts

    def steps(shift, chunk, begin):
        far = max(0, abs(shift) * group - (group - 1))
        other = unit + shift
        most = min(MAX_WIDTH[min(far, RADIUS)], blocks)
        for member in range(group):
            qf = frame_of(unit, place, group, member)
            order = [member] + [i for i in range(group) if i != member]
            batches = [[i] for i in order] if most == blocks else [order]
            for index, batch in enumerate(batches):
                for head in range(heads):
                    for b in range(blocks):
                        found = []
                        for i in batch:
                            kf = frame_of(other, place, group, i)
                            found += pair_slots(b, qf, kf, far, i, chunk[i])
                        key_slots = jnp.concatenate(gather(found, head, 0), axis=0)
                        value_slots = jnp.concatenate(
                            [
                                jnp.concatenate([v, ones], axis=1)
                                for v in gather(found, head, width)
                            ],
                            axis=0,
                        )
                        rows = slice(member * tokens + b * BLK, member * tokens + (b + 1) * BLK)
                        query = q_refs[member][
                            b * BLK : (b + 1) * BLK, head * HEAD : (head + 1) * HEAD
                        ]
                        oks = [ok for _, _, ok in found]
                        update(
                            b, rows, query, key_slots, value_slots, oks,
                            m_ref, acc_ref, head, begin and index == 0,
                        )

    for shift, chunk in zip(shifts, chunks):
        if shift == 0:
            steps(shift, chunk, begins)
        else:
            other = unit + shift

            @pl.when((other >= 0) & (other < units))
            def _(shift=shift, chunk=chunk):
                steps(shift, chunk, False)

    if ends:
        for member in range(group):
            start = (place if member == 0 else group - 1 - place) * tokens
            for head in range(heads):
                for b in range(blocks):
                    rows = slice(member * tokens + b * BLK, member * tokens + (b + 1) * BLK)
                    both = acc_ref[head, rows, :]
                    at = pl.ds(pl.multiple_of(start + b * BLK, BLK), BLK)
                    out_ref[at, head * HEAD : (head + 1) * HEAD] = (
                        both[:, :HEAD] / both[:, HEAD:]
                    ).astype(out_ref.dtype)


def attend(cfg, bands, queries, chunks, state):
    group, heads, shifts, units, begins, ends = cfg
    tokens = queries[0].shape[0]
    rows = group * tokens
    m_shape = pltpu.VMEM((heads, rows, BLK), jnp.float32)
    acc_shape = pltpu.VMEM((heads, rows, 2 * HEAD), jnp.float32)
    flat = [in_vmem(c) for pair in chunks for c in pair]
    inputs = [*bands, *[in_vmem(q) for q in queries], *flat, *state]
    outs = [m_shape, acc_shape]
    aliases = {}
    if not begins:
        aliases = {len(inputs) - 2: 0, len(inputs) - 1: 1}
    if ends:
        outs = [pltpu.VMEM((rows, heads * HEAD), queries[0].dtype), m_shape, acc_shape]
        aliases = {index: out + 1 for index, out in aliases.items()}
    work = 4 * len(flat) * tokens * rows * heads * HEAD
    return pl.pallas_call(
        functools.partial(attend_kernel, cfg),
        out_shape=outs,
        in_specs=[SMEM] * 2 + [VMEM] * (len(inputs) - 2),
        out_specs=[VMEM] * len(outs),
        input_output_aliases=aliases,
        compiler_params=params(),
        cost_estimate=pl.CostEstimate(flops=work, bytes_accessed=1 << 20, transcendentals=0),
        name="attend_" + "_".join(str(abs(s)) for s in shifts),
    )(*inputs)


def project_kernel(group, ranks, rows_ref, *refs):
    weights, out_ref = refs[:-1], refs[-1]
    me = lax.axis_index("head")
    total = None
    for offset, weight in enumerate(weights):
        owner = me ^ offset
        left = jnp.concatenate([rows_ref[i * ranks + owner] for i in range(group)], axis=1)
        term = jnp.dot(left, weight[...], preferred_element_type=jnp.float32)
        total = term if total is None else total + term
    out_ref[...] = total.astype(out_ref.dtype)


def project(rows, weights, group):
    ranks = len(weights)
    tokens, columns = rows.shape[1], weights[0].shape[1]
    return pl.pallas_call(
        functools.partial(project_kernel, group, ranks),
        out_shape=jax.ShapeDtypeStruct((tokens, columns), rows.dtype),
        in_specs=[VMEM] * (1 + ranks),
        out_specs=VMEM,
        compiler_params=params(),
        cost_estimate=pl.CostEstimate(
            flops=2 * rows.size * columns, bytes_accessed=1 << 20, transcendentals=0
        ),
        name="project",
    )(in_vmem(rows), *[in_vmem(w) for w in weights])


def on_device(queries, keys, values, band_width, band_offset, out_weight):
    frames, ranks = lax.axis_size("frame"), lax.axis_size("head")
    tokens = queries.shape[0]
    local_heads = queries.shape[1] // HEAD
    group = 2 if local_heads % 2 == 0 and frames % 2 == 0 else 1
    heads = local_heads // group
    units = frames // group

    def along(value, steps):
        sources = [s for s in steps]
        pairs = [(a * group + i, b * group + i) for a, b in sources for i in range(group)]
        return lax.ppermute(value, "frame", pairs)

    pieces = split(queries, keys, values, group)
    own, own_queries = pieces[0], pieces[1]
    chunks, query_rows = [own], [own_queries]
    if group == 2:
        swap = [(f, f ^ 1) for f in range(frames)]
        chunks.append(lax.ppermute(pieces[2], "frame", swap))
        query_rows.append(lax.ppermute(pieces[3], "frame", swap))

    weights = {0: out_weight}
    bit = ranks // 2
    while bit:
        for offset in list(weights):
            pairs = [(h, h ^ bit) for h in range(ranks)]
            weights[offset ^ bit] = lax.ppermute(weights[offset], "head", pairs)
        bit //= 2
    weights = [weights[o] for o in range(ranks)]

    furthest = min(units - 1, (RADIUS + group - 1) // group)
    bands = (band_width, band_offset)
    lower, upper = chunks, chunks
    arrived = []
    for k in range(1, furthest + 1):
        up = [(s, s + 1) for s in range(k - 1, units - 1)]
        down = [(s, s - 1) for s in range(1, units - k + 1)]
        pairs = [(along(a, up), along(b, down)) for a, b in zip(lower, upper)]
        lower, upper = [p[0] for p in pairs], [p[1] for p in pairs]
        arrived.append((lower, upper))

    state = attend((group, heads, (0,), units, True, False), bands, query_rows, [chunks], [])
    for k, (lower, upper) in enumerate(arrived, 1):
        cfg = (group, heads, (-k, k), units, False, k == furthest)
        state = attend(cfg, bands, query_rows, [lower, upper], state)
    attended = state[0]

    members = [
        [(u * group + i) * ranks + h for i in range(group) for h in range(ranks)]
        for u in range(units)
    ]
    blocks = attended.reshape(group * ranks, tokens // ranks, heads * HEAD)
    rows = lax.all_to_all(
        blocks, ("frame", "head"), split_axis=0, concat_axis=0, tiled=True,
        axis_index_groups=members,
    )
    return project(rows, weights, group)


def solution(mesh):
    placed = (P("frame", "head"), P("frame", "head"), P("frame", "head"), P(), P(), P("head", None))
    return jax.shard_map(
        on_device, mesh=mesh, in_specs=placed, out_specs=P(("frame", "head"), None), check_vma=False
    )
```

```python
import functools
import math

import jax
import jax.numpy as jnp
from jax import lax
from jax.experimental import pallas as pl
from jax.experimental.pallas import tpu as pltpu
from jax.sharding import PartitionSpec as P


HEAD = 128
BLK = 128
RADIUS = 7
MAX_WIDTH = (4, 4, 2, 2, 1, 1, 1, 1)
MASKED = -1e30
EXPONENT = math.log2(math.e) / math.sqrt(HEAD)

VMEM = pl.BlockSpec(memory_space=pltpu.VMEM)
SMEM = pl.BlockSpec(memory_space=pltpu.SMEM)
HBM = pl.BlockSpec(memory_space=pltpu.HBM)


def in_vmem(value):
    return pltpu.with_memory_space_constraint(value, pltpu.VMEM)


def in_hbm(value):
    return pltpu.with_memory_space_constraint(value, pltpu.HBM)


def params():
    return pltpu.CompilerParams(vmem_limit_bytes=32 << 20)


def split_kernel(group, q_ref, k_ref, v_ref, width_ref, offset_ref, *refs):
    outs, sem = refs[:-1], refs[-1]
    width = outs[0].shape[1] // 2
    place = lax.rem(lax.axis_index("frame"), group)
    copies = []
    for part in range(group):
        column = (place if part == 0 else 1 - place) * width
        columns = pl.ds(pl.multiple_of(column, HEAD), width)
        pair, rows = outs[2 * part], outs[2 * part + 1]
        for source, target in (
            (k_ref, pair.at[:, :width]),
            (v_ref, pair.at[:, width:]),
            (q_ref, rows),
        ):
            copies.append(
                pltpu.make_async_copy(source.at[:, columns], target, sem.at[len(copies)])
            )
    for source, target in ((width_ref, outs[-2]), (offset_ref, outs[-1])):
        copies.append(pltpu.make_async_copy(source, target, sem.at[len(copies)]))
    for copy in copies:
        copy.start()
    for copy in copies:
        copy.wait()


def split(queries, keys, values, bands, group):
    tokens, columns = queries.shape
    width = columns // group
    pair = pltpu.VMEM((tokens, 2 * width), queries.dtype)
    rows = pltpu.VMEM((tokens, width), queries.dtype)
    return pl.pallas_call(
        functools.partial(split_kernel, group),
        out_shape=[pair, rows] * group + [pltpu.SMEM(b.shape, b.dtype) for b in bands],
        in_specs=[HBM] * 5,
        out_specs=[VMEM] * (2 * group) + [SMEM] * 2,
        scratch_shapes=[pltpu.SemaphoreType.DMA((3 * group + 2,))],
        compiler_params=params(),
        name="split",
    )(*[in_hbm(v) for v in (queries, keys, values, *bands)])


def frame_of(unit, place, group, member):
    return unit * group + (place if member == 0 else group - 1 - place)


def update(rows, query, key_slots, value_slots, oks, m_ref, acc_ref, head, first):
    scores = lax.dot_general(
        query, key_slots, (((1,), (1,)), ((), ())), preferred_element_type=jnp.float32
    )
    pieces = [scores[:, BLK * j : BLK * (j + 1)] for j in range(len(oks))]
    pieces = [s if ok is None else jnp.where(ok, s, MASKED) for s, ok in zip(pieces, oks)]
    tallest = functools.reduce(jnp.maximum, pieces)
    tallest = jnp.max(tallest, axis=1, keepdims=True)
    if first:
        peak = jnp.broadcast_to(tallest, (BLK, BLK))
    else:
        before = m_ref[head, rows, :]
        peak = jnp.maximum(before, tallest)
    weights = [jnp.exp2((s - peak) * EXPONENT).astype(jnp.bfloat16) for s in pieces]
    weights = jnp.concatenate(weights, axis=1)
    added = jnp.dot(weights, value_slots, preferred_element_type=jnp.float32)
    if not first:
        rescale = jnp.exp2((before - peak) * EXPONENT)
        rescale = jnp.concatenate([rescale, rescale], axis=1)
        added = acc_ref[head, rows, :] * rescale + added
    acc_ref[head, rows, :] = added
    m_ref[head, rows, :] = peak


def attend_kernel(cfg, width_ref, offset_ref, *refs):
    group, heads, shifts, units, begins, ends = cfg
    q_refs, refs = refs[:group], refs[group:]
    chunks = [refs[group * i : group * (i + 1)] for i in range(len(shifts))]
    refs = refs[group * len(shifts) :]
    if not begins:
        refs = refs[2:]
    if ends:
        out_ref, m_ref, acc_ref = refs
    else:
        m_ref, acc_ref = refs
    tokens = q_refs[0].shape[0]
    blocks = tokens // BLK
    width = heads * HEAD
    me = lax.axis_index("frame")
    unit, place = me // group, lax.rem(me, group)
    ones = jnp.ones((BLK, HEAD), jnp.bfloat16)

    def pair_slots(b, qf, kf, far, refs):
        distance = jnp.abs(qf - kf)
        present = distance <= RADIUS
        reach = jnp.minimum(distance, RADIUS)
        span = width_ref[qf, reach]
        start = offset_ref[qf, b, reach]
        most = min(MAX_WIDTH[min(far, RADIUS)], blocks)
        found = []
        for j in range(most):
            if most == blocks:
                inside = lax.rem(j - start + blocks, blocks) < span
                if far == 0:
                    inside = inside | ((distance == 0) & (b == j))
                found.append((refs, j, present & inside))
            else:
                inside = None if most == 1 and far * 1 <= RADIUS - 2 * (group - 1) else present & (j < span)
                found.append((refs, lax.rem(start + j, blocks), inside))
        return found

    def gather(found, head, column):
        parts = []
        for ref, block, _ in found:
            if isinstance(block, int):
                at = pl.ds(block * BLK, BLK)
            else:
                at = pl.ds(pl.multiple_of(block * BLK, BLK), BLK)
            parts.append(ref[at, column + head * HEAD : column + (head + 1) * HEAD])
        return parts

    def steps(shift, chunk, begin):
        far = max(0, abs(shift) * group - (group - 1))
        other = unit + shift
        most = min(MAX_WIDTH[min(far, RADIUS)], blocks)
        for member in range(group):
            qf = frame_of(unit, place, group, member)
            order = [member] + [i for i in range(group) if i != member]
            batches = [[i] for i in order] if most == blocks else [order]
            for index, batch in enumerate(batches):
                for head in range(heads):
                    for b in range(blocks):
                        found = []
                        for i in batch:
                            kf = frame_of(other, place, group, i)
                            found += pair_slots(b, qf, kf, far, chunk[i])
                        key_slots = jnp.concatenate(gather(found, head, 0), axis=0)
                        value_slots = jnp.concatenate(
                            [
                                jnp.concatenate([v, ones], axis=1)
                                for v in gather(found, head, width)
                            ],
                            axis=0,
                        )
                        rows = slice(member * tokens + b * BLK, member * tokens + (b + 1) * BLK)
                        query = q_refs[member][
                            b * BLK : (b + 1) * BLK, head * HEAD : (head + 1) * HEAD
                        ]
                        oks = [ok for _, _, ok in found]
                        update(
                            rows, query, key_slots, value_slots, oks,
                            m_ref, acc_ref, head, begin and index == 0,
                        )

    for shift, chunk in zip(shifts, chunks):
        if shift == 0:
            steps(shift, chunk, begins)
        else:
            other = unit + shift

            @pl.when((other >= 0) & (other < units))
            def _(shift=shift, chunk=chunk):
                steps(shift, chunk, False)

    if ends:
        for member in range(group):
            start = (place if member == 0 else group - 1 - place) * tokens
            for head in range(heads):
                for b in range(blocks):
                    rows = slice(member * tokens + b * BLK, member * tokens + (b + 1) * BLK)
                    both = acc_ref[head, rows, :]
                    at = pl.ds(pl.multiple_of(start + b * BLK, BLK), BLK)
                    out_ref[at, head * HEAD : (head + 1) * HEAD] = (
                        both[:, :HEAD] / both[:, HEAD:]
                    ).astype(out_ref.dtype)


def attend(cfg, bands, queries, chunks, state):
    group, heads, _, _, begins, ends = cfg
    tokens = queries[0].shape[0]
    rows = group * tokens
    m_shape = pltpu.VMEM((heads, rows, BLK), jnp.float32)
    acc_shape = pltpu.VMEM((heads, rows, 2 * HEAD), jnp.float32)
    flat = [in_vmem(c) for pair in chunks for c in pair]
    inputs = [*bands, *[in_vmem(q) for q in queries], *flat, *state]
    outs = [m_shape, acc_shape]
    aliases = {}
    if not begins:
        aliases = {len(inputs) - 2: 0, len(inputs) - 1: 1}
    if ends:
        outs = [jax.ShapeDtypeStruct((rows, heads * HEAD), queries[0].dtype), m_shape, acc_shape]
        aliases = {index: out + 1 for index, out in aliases.items()}
    work = 4 * len(flat) * tokens * rows * heads * HEAD
    return pl.pallas_call(
        functools.partial(attend_kernel, cfg),
        out_shape=outs,
        in_specs=[SMEM] * 2 + [VMEM] * (len(inputs) - 2),
        out_specs=[VMEM] * len(outs),
        input_output_aliases=aliases,
        compiler_params=params(),
        cost_estimate=pl.CostEstimate(flops=work, bytes_accessed=1 << 20, transcendentals=0),
    )(*inputs)


def project_kernel(group, ranks, rows_ref, *refs):
    weights, out_ref = refs[:-1], refs[-1]
    me = lax.axis_index("head")
    total = None
    for offset, weight in enumerate(weights):
        owner = me ^ offset
        left = jnp.concatenate([rows_ref[i * ranks + owner] for i in range(group)], axis=1)
        term = jnp.dot(left, weight[...], preferred_element_type=jnp.float32)
        total = term if total is None else total + term
    out_ref[...] = total.astype(out_ref.dtype)


def project(rows, weights, group):
    ranks = len(weights)
    tokens, columns = rows.shape[1], weights[0].shape[1]
    return pl.pallas_call(
        functools.partial(project_kernel, group, ranks),
        out_shape=jax.ShapeDtypeStruct((tokens, columns), rows.dtype),
        in_specs=[VMEM] * (1 + ranks),
        out_specs=VMEM,
        compiler_params=params(),
        cost_estimate=pl.CostEstimate(
            flops=2 * rows.size * columns, bytes_accessed=1 << 20, transcendentals=0
        ),
        name="project",
    )(in_vmem(rows), *[in_vmem(w) for w in weights])


def plan(shape, columns):
    frames, local_heads = shape["frame"], columns // HEAD
    group = 2 if local_heads % 2 == 0 and frames % 2 == 0 else 1
    units = frames // group
    return group, units, min(units - 1, (RADIUS + group - 1) // group)


def on_device(queries, keys, values, band_width, band_offset, out_weight):
    frames, ranks = lax.axis_size("frame"), lax.axis_size("head")
    tokens = queries.shape[0]
    group, units, furthest = plan({"frame": frames}, queries.shape[1])
    heads = queries.shape[1] // HEAD // group

    def along(value, steps):
        pairs = [(a * group + i, b * group + i) for a, b in steps for i in range(group)]
        return lax.ppermute(value, "frame", pairs)

    bands = (band_width, jnp.transpose(band_offset, (0, 2, 1)))
    *pieces, band_width, band_offset = split(queries, keys, values, bands, group)
    bands = (band_width, band_offset)
    chunks, query_rows = [pieces[0]], [pieces[1]]
    if group == 2:
        swap = [(f, f ^ 1) for f in range(frames)]
        chunks.append(lax.ppermute(pieces[2], "frame", swap))
        query_rows.append(lax.ppermute(pieces[3], "frame", swap))

    weights = {0: out_weight}
    bit = ranks // 2
    while bit:
        for offset in list(weights):
            pairs = [(h, h ^ bit) for h in range(ranks)]
            weights[offset ^ bit] = lax.ppermute(weights[offset], "head", pairs)
        bit //= 2
    weights = [weights[o] for o in range(ranks)]

    lower, upper = chunks, chunks
    arrived = []
    for k in range(1, furthest + 1):
        up = [(s, s + 1) for s in range(k - 1, units - 1)]
        down = [(s, s - 1) for s in range(1, units - k + 1)]
        lower = [along(c, up) for c in lower]
        upper = [along(c, down) for c in upper]
        arrived.append((lower, upper))

    cfg = (group, heads, (0,), units, True, False)
    state = attend(cfg, bands, query_rows, [chunks], [])
    for k, (lower, upper) in enumerate(arrived, 1):
        cfg = (group, heads, (-k, k), units, False, k == furthest)
        state = attend(cfg, bands, query_rows, [lower, upper], state)
    attended = state[0]

    members = [
        [(u * group + i) * ranks + h for i in range(group) for h in range(ranks)]
        for u in range(units)
    ]
    blocks = attended.reshape(group * ranks, tokens // ranks, heads * HEAD)
    rows = lax.all_to_all(
        blocks, ("frame", "head"), split_axis=0, concat_axis=0, tiled=True,
        axis_index_groups=members,
    )
    return project(rows, weights, group)


def solution(mesh):
    placed = (P("frame", "head"), P("frame", "head"), P("frame", "head"), P(), P(), P("head", None))
    return jax.shard_map(
        on_device, mesh=mesh, in_specs=placed, out_specs=P(("frame", "head"), None), check_vma=False
    )
```

```python
import functools
import math

import jax
import jax.numpy as jnp
from jax import lax
from jax.experimental import pallas as pl
from jax.experimental.pallas import tpu as pltpu
from jax.sharding import PartitionSpec as P


HEAD = 128
BLK = 128
RADIUS = 7
MAX_WIDTH = (4, 4, 2, 2, 1, 1, 1, 1)
MASKED = -1e30
EXPONENT = math.log2(math.e) / math.sqrt(HEAD)

VMEM = pl.BlockSpec(memory_space=pltpu.VMEM)
SMEM = pl.BlockSpec(memory_space=pltpu.SMEM)
HBM = pl.BlockSpec(memory_space=pltpu.HBM)


def in_vmem(value):
    return pltpu.with_memory_space_constraint(value, pltpu.VMEM)


def in_hbm(value):
    return pltpu.with_memory_space_constraint(value, pltpu.HBM)


def params():
    return pltpu.CompilerParams(vmem_limit_bytes=32 << 20)


def split_kernel(group, q_ref, k_ref, v_ref, width_ref, offset_ref, *refs):
    outs, sem = refs[:-1], refs[-1]
    width = outs[0].shape[1] // 2
    place = lax.rem(lax.axis_index("frame"), group)
    copies = []
    for part in range(group):
        column = (place if part == 0 else 1 - place) * width
        columns = pl.ds(pl.multiple_of(column, HEAD), width)
        pair, rows = outs[2 * part], outs[2 * part + 1]
        for source, target in (
            (k_ref, pair.at[:, :width]),
            (v_ref, pair.at[:, width:]),
            (q_ref, rows),
        ):
            copies.append(
                pltpu.make_async_copy(source.at[:, columns], target, sem.at[len(copies)])
            )
    for source, target in ((width_ref, outs[-2]), (offset_ref, outs[-1])):
        copies.append(pltpu.make_async_copy(source, target, sem.at[len(copies)]))
    for copy in copies:
        copy.start()
    for copy in copies:
        copy.wait()


def split(queries, keys, values, bands, group):
    tokens, columns = queries.shape
    width = columns // group
    pair = pltpu.VMEM((tokens, 2 * width), queries.dtype)
    rows = pltpu.VMEM((tokens, width), queries.dtype)
    return pl.pallas_call(
        functools.partial(split_kernel, group),
        out_shape=[pair, rows] * group + [pltpu.SMEM(b.shape, b.dtype) for b in bands],
        in_specs=[HBM] * 5,
        out_specs=[VMEM] * (2 * group) + [SMEM] * 2,
        scratch_shapes=[pltpu.SemaphoreType.DMA((3 * group + 2,))],
        compiler_params=params(),
        name="split",
    )(*[in_hbm(v) for v in (queries, keys, values, *bands)])


def frame_of(unit, place, group, member):
    return unit * group + (place if member == 0 else group - 1 - place)


def update(rows, query, key_slots, value_slots, oks, m_ref, acc_ref, head, first):
    scores = lax.dot_general(
        query, key_slots, (((1,), (1,)), ((), ())), preferred_element_type=jnp.float32
    )
    pieces = [scores[:, BLK * j : BLK * (j + 1)] for j in range(len(oks))]
    pieces = [s if ok is None else jnp.where(ok, s, MASKED) for s, ok in zip(pieces, oks)]
    tallest = functools.reduce(jnp.maximum, pieces)
    tallest = jnp.max(tallest, axis=1, keepdims=True)
    if first:
        peak = jnp.broadcast_to(tallest, (BLK, BLK))
    else:
        before = m_ref[head, rows, :]
        peak = jnp.maximum(before, tallest)
    weights = [jnp.exp2((s - peak) * EXPONENT).astype(jnp.bfloat16) for s in pieces]
    weights = jnp.concatenate(weights, axis=1)
    added = jnp.dot(weights, value_slots, preferred_element_type=jnp.float32)
    if not first:
        rescale = jnp.exp2((before - peak) * EXPONENT)
        rescale = jnp.concatenate([rescale, rescale], axis=1)
        added = acc_ref[head, rows, :] * rescale + added
    acc_ref[head, rows, :] = added
    m_ref[head, rows, :] = peak


def attend_kernel(cfg, width_ref, offset_ref, *refs):
    group, heads, shifts, units, begins, ends = cfg
    q_refs, refs = refs[:group], refs[group:]
    chunks = [refs[group * i : group * (i + 1)] for i in range(len(shifts))]
    refs = refs[group * len(shifts) :]
    if not begins:
        refs = refs[2:]
    if ends:
        out_ref, m_ref, acc_ref = refs
    else:
        m_ref, acc_ref = refs
    tokens = q_refs[0].shape[0]
    blocks = tokens // BLK
    width = heads * HEAD
    me = lax.axis_index("frame")
    unit, place = me // group, lax.rem(me, group)
    ones = jnp.ones((BLK, HEAD), jnp.bfloat16)

    def pair_slots(b, qf, kf, far, refs):
        distance = jnp.abs(qf - kf)
        present = distance <= RADIUS
        reach = jnp.minimum(distance, RADIUS)
        span = width_ref[qf, reach]
        start = offset_ref[qf, b, reach]
        most = min(MAX_WIDTH[min(far, RADIUS)], blocks)
        found = []
        for j in range(most):
            if most == blocks:
                inside = lax.rem(j - start + blocks, blocks) < span
                if far == 0:
                    inside = inside | ((distance == 0) & (b == j))
                found.append((refs, j, present & inside))
            else:
                inside = None if most == 1 and far * 1 <= RADIUS - 2 * (group - 1) else present & (j < span)
                found.append((refs, lax.rem(start + j, blocks), inside))
        return found

    def gather(found, head, column):
        parts = []
        for ref, block, _ in found:
            if isinstance(block, int):
                at = pl.ds(block * BLK, BLK)
            else:
                at = pl.ds(pl.multiple_of(block * BLK, BLK), BLK)
            parts.append(ref[at, column + head * HEAD : column + (head + 1) * HEAD])
        return parts

    def steps(step, other, chunk, begin):
        far = max(0, step * group - (group - 1))
        most = min(MAX_WIDTH[min(far, RADIUS)], blocks)
        for member in range(group):
            qf = frame_of(unit, place, group, member)
            order = [member] + [i for i in range(group) if i != member]
            batches = [[i] for i in order] if most == blocks else [order]
            for index, batch in enumerate(batches):
                for head in range(heads):
                    for b in range(blocks):
                        found = []
                        for i in batch:
                            kf = frame_of(other, place, group, i)
                            found += pair_slots(b, qf, kf, far, chunk[i])
                        key_slots = jnp.concatenate(gather(found, head, 0), axis=0)
                        value_slots = jnp.concatenate(
                            [
                                jnp.concatenate([v, ones], axis=1)
                                for v in gather(found, head, width)
                            ],
                            axis=0,
                        )
                        rows = slice(member * tokens + b * BLK, member * tokens + (b + 1) * BLK)
                        query = q_refs[member][
                            b * BLK : (b + 1) * BLK, head * HEAD : (head + 1) * HEAD
                        ]
                        oks = [ok for _, _, ok in found]
                        update(
                            rows, query, key_slots, value_slots, oks,
                            m_ref, acc_ref, head, begin and index == 0,
                        )

    facing = 1 - 2 * lax.rem(unit, 2)
    for (step, parity), chunk in zip(shifts, chunks):
        if step == 0:
            steps(0, unit, chunk, begins)
        else:
            other = unit + step * (facing if parity == 0 else -facing)

            @pl.when((other >= 0) & (other < units))
            def _(step=step, other=other, chunk=chunk):
                steps(step, other, chunk, False)

    if ends:
        for member in range(group):
            start = (place if member == 0 else group - 1 - place) * tokens
            for head in range(heads):
                for b in range(blocks):
                    rows = slice(member * tokens + b * BLK, member * tokens + (b + 1) * BLK)
                    both = acc_ref[head, rows, :]
                    at = pl.ds(pl.multiple_of(start + b * BLK, BLK), BLK)
                    out_ref[at, head * HEAD : (head + 1) * HEAD] = (
                        both[:, :HEAD] / both[:, HEAD:]
                    ).astype(out_ref.dtype)


def attend(cfg, bands, queries, chunks, state):
    group, heads, _, _, begins, ends = cfg
    tokens = queries[0].shape[0]
    rows = group * tokens
    m_shape = pltpu.VMEM((heads, rows, BLK), jnp.float32)
    acc_shape = pltpu.VMEM((heads, rows, 2 * HEAD), jnp.float32)
    flat = [in_vmem(c) for pair in chunks for c in pair]
    inputs = [*bands, *[in_vmem(q) for q in queries], *flat, *state]
    outs = [m_shape, acc_shape]
    aliases = {}
    if not begins:
        aliases = {len(inputs) - 2: 0, len(inputs) - 1: 1}
    if ends:
        outs = [jax.ShapeDtypeStruct((rows, heads * HEAD), queries[0].dtype), m_shape, acc_shape]
        aliases = {index: out + 1 for index, out in aliases.items()}
    work = 4 * len(flat) * tokens * rows * heads * HEAD
    return pl.pallas_call(
        functools.partial(attend_kernel, cfg),
        out_shape=outs,
        in_specs=[SMEM] * 2 + [VMEM] * (len(inputs) - 2),
        out_specs=[VMEM] * len(outs),
        input_output_aliases=aliases,
        compiler_params=params(),
        cost_estimate=pl.CostEstimate(flops=work, bytes_accessed=1 << 20, transcendentals=0),
    )(*inputs)


def project_kernel(group, ranks, rows_ref, *refs):
    weights, out_ref = refs[:-1], refs[-1]
    me = lax.axis_index("head")
    total = None
    for offset, weight in enumerate(weights):
        owner = me ^ offset
        left = jnp.concatenate([rows_ref[i * ranks + owner] for i in range(group)], axis=1)
        term = jnp.dot(left, weight[...], preferred_element_type=jnp.float32)
        total = term if total is None else total + term
    out_ref[...] = total.astype(out_ref.dtype)


def project(rows, weights, group):
    ranks = len(weights)
    tokens, columns = rows.shape[1], weights[0].shape[1]
    return pl.pallas_call(
        functools.partial(project_kernel, group, ranks),
        out_shape=jax.ShapeDtypeStruct((tokens, columns), rows.dtype),
        in_specs=[VMEM] * (1 + ranks),
        out_specs=VMEM,
        compiler_params=params(),
        cost_estimate=pl.CostEstimate(
            flops=2 * rows.size * columns, bytes_accessed=1 << 20, transcendentals=0
        ),
        name="project",
    )(in_vmem(rows), *[in_vmem(w) for w in weights])


def plan(shape, columns):
    frames, local_heads = shape["frame"], columns // HEAD
    group = 2 if local_heads % 2 == 0 and frames % 2 == 0 else 1
    units = frames // group
    return group, units, min(units - 1, (RADIUS + group - 1) // group)


def edges(units, k, parity):
    sends = []
    for low in range(parity, units - 1, 2):
        if low + 1 - k >= 0:
            sends.append((low, low + 1))
        if low + k < units:
            sends.append((low + 1, low))
    return sends


def on_device(queries, keys, values, band_width, band_offset, out_weight):
    frames, ranks = lax.axis_size("frame"), lax.axis_size("head")
    tokens = queries.shape[0]
    group, units, furthest = plan({"frame": frames}, queries.shape[1])
    heads = queries.shape[1] // HEAD // group

    def along(value, steps):
        pairs = [(a * group + i, b * group + i) for a, b in steps for i in range(group)]
        return lax.ppermute(value, "frame", pairs)

    bands = (band_width, jnp.transpose(band_offset, (0, 2, 1)))
    *pieces, band_width, band_offset = split(queries, keys, values, bands, group)
    bands = (band_width, band_offset)
    chunks, query_rows = [pieces[0]], [pieces[1]]
    if group == 2:
        swap = [(f, f ^ 1) for f in range(frames)]
        chunks.append(lax.ppermute(pieces[2], "frame", swap))
        query_rows.append(lax.ppermute(pieces[3], "frame", swap))

    weights = {0: out_weight}
    bit = ranks // 2
    while bit:
        for offset in list(weights):
            pairs = [(h, h ^ bit) for h in range(ranks)]
            weights[offset ^ bit] = lax.ppermute(weights[offset], "head", pairs)
        bit //= 2
    weights = [weights[o] for o in range(ranks)]

    held, arrived = [chunks, chunks], []
    for k in range(1, furthest + 1):
        held = [
            [along(c, edges(units, k, parity)) for c in source]
            for parity, source in enumerate(reversed(held))
            if edges(units, k, parity)
        ]
        arrived.append(held)

    cfg = (group, heads, ((0, 0),), units, True, False)
    state = attend(cfg, bands, query_rows, [chunks], [])
    for k, received in enumerate(arrived, 1):
        shifts = tuple((k, parity) for parity in range(2) if edges(units, k, parity))
        cfg = (group, heads, shifts, units, False, k == furthest)
        state = attend(cfg, bands, query_rows, received, state)
    attended = state[0]

    members = [
        [(u * group + i) * ranks + h for i in range(group) for h in range(ranks)]
        for u in range(units)
    ]
    blocks = attended.reshape(group * ranks, tokens // ranks, heads * HEAD)
    rows = lax.all_to_all(
        blocks, ("frame", "head"), split_axis=0, concat_axis=0, tiled=True,
        axis_index_groups=members,
    )
    return project(rows, weights, group)


def solution(mesh):
    placed = (P("frame", "head"), P("frame", "head"), P("frame", "head"), P(), P(), P("head", None))
    return jax.shard_map(
        on_device, mesh=mesh, in_specs=placed, out_specs=P(("frame", "head"), None), check_vma=False
    )
```

```python
import functools
import math

import jax
import jax.numpy as jnp
from jax import lax
from jax.experimental import pallas as pl
from jax.experimental.pallas import tpu as pltpu
from jax.sharding import PartitionSpec as P


HEAD = 128
BLK = 128
RADIUS = 7
MAX_WIDTH = (4, 4, 2, 2, 1, 1, 1, 1)
MASKED = -1e30
EXPONENT = math.log2(math.e) / math.sqrt(HEAD)

VMEM = pl.BlockSpec(memory_space=pltpu.VMEM)
SMEM = pl.BlockSpec(memory_space=pltpu.SMEM)
HBM = pl.BlockSpec(memory_space=pltpu.HBM)


def in_vmem(value):
    return pltpu.with_memory_space_constraint(value, pltpu.VMEM)


def in_hbm(value):
    return pltpu.with_memory_space_constraint(value, pltpu.HBM)


def params():
    return pltpu.CompilerParams(vmem_limit_bytes=32 << 20)


def split_kernel(group, q_ref, k_ref, v_ref, width_ref, offset_ref, *refs):
    outs, sem = refs[:-1], refs[-1]
    width = outs[0].shape[1] // 2
    place = lax.rem(lax.axis_index("frame"), group)
    copies = []
    for part in range(group):
        column = (place if part == 0 else 1 - place) * width
        columns = pl.ds(pl.multiple_of(column, HEAD), width)
        pair, rows = outs[2 * part], outs[2 * part + 1]
        for source, target in (
            (k_ref, pair.at[:, :width]),
            (v_ref, pair.at[:, width:]),
            (q_ref, rows),
        ):
            copies.append(
                pltpu.make_async_copy(source.at[:, columns], target, sem.at[len(copies)])
            )
    for source, target in ((width_ref, outs[-2]), (offset_ref, outs[-1])):
        copies.append(pltpu.make_async_copy(source, target, sem.at[len(copies)]))
    for copy in copies:
        copy.start()
    for copy in copies:
        copy.wait()


def split(queries, keys, values, bands, group):
    tokens, columns = queries.shape
    width = columns // group
    pair = pltpu.VMEM((tokens, 2 * width), queries.dtype)
    rows = pltpu.VMEM((tokens, width), queries.dtype)
    return pl.pallas_call(
        functools.partial(split_kernel, group),
        out_shape=[pair, rows] * group + [pltpu.SMEM(b.shape, b.dtype) for b in bands],
        in_specs=[HBM] * 5,
        out_specs=[VMEM] * (2 * group) + [SMEM] * 2,
        scratch_shapes=[pltpu.SemaphoreType.DMA((3 * group + 2,))],
        compiler_params=params(),
        name="split",
    )(*[in_hbm(v) for v in (queries, keys, values, *bands)])


def frame_of(unit, place, group, member):
    return unit * group + (place if member == 0 else group - 1 - place)


def update(rows, query, key_slots, value_slots, oks, m_ref, acc_ref, head, first):
    scores = lax.dot_general(
        query, key_slots, (((1,), (1,)), ((), ())), preferred_element_type=jnp.float32
    )
    pieces = [scores[:, BLK * j : BLK * (j + 1)] for j in range(len(oks))]
    pieces = [s if ok is None else jnp.where(ok, s, MASKED) for s, ok in zip(pieces, oks)]
    tallest = functools.reduce(jnp.maximum, pieces)
    tallest = jnp.max(tallest, axis=1, keepdims=True)
    if first:
        peak = jnp.broadcast_to(tallest, (BLK, BLK))
    else:
        before = m_ref[head, rows, :]
        peak = jnp.maximum(before, tallest)
    weights = [jnp.exp2((s - peak) * EXPONENT).astype(jnp.bfloat16) for s in pieces]
    weights = jnp.concatenate(weights, axis=1)
    added = jnp.dot(weights, value_slots, preferred_element_type=jnp.float32)
    if not first:
        rescale = jnp.exp2((before - peak) * EXPONENT)
        rescale = jnp.concatenate([rescale, rescale], axis=1)
        added = acc_ref[head, rows, :] * rescale + added
    acc_ref[head, rows, :] = added
    m_ref[head, rows, :] = peak


def unit_at(spec, unit, units):
    kind, step, parity = spec
    if kind == "own":
        return unit, None
    if kind == "edge":
        facing = 1 - 2 * lax.rem(unit, 2)
        other = unit + step * (facing if parity == 0 else -facing)
        return other, (other >= 0) & (other < units)
    inwards = jnp.where(2 * unit < units, 1, -1)
    return unit + step * inwards, (unit > 0) & (unit < units - 1)


def attend_kernel(cfg, width_ref, offset_ref, *refs):
    group, heads, units, queries, keys, jobs, begins, ends = cfg
    q_sets = [refs[group * i : group * (i + 1)] for i in range(len(queries))]
    refs = refs[group * len(queries) :]
    chunks = [refs[group * i : group * (i + 1)] for i in range(len(keys))]
    refs = refs[group * len(keys) :]
    if not begins:
        refs = refs[2:]
    if ends:
        out_ref, m_ref, acc_ref = refs
    else:
        m_ref, acc_ref = refs
    tokens = q_sets[0][0].shape[0]
    blocks = tokens // BLK
    width = heads * HEAD
    me = lax.axis_index("frame")
    unit, place = me // group, lax.rem(me, group)
    ones = jnp.ones((BLK, HEAD), jnp.bfloat16)

    def pair_slots(b, qf, kf, far, refs):
        distance = jnp.abs(qf - kf)
        present = distance <= RADIUS
        reach = jnp.minimum(distance, RADIUS)
        span = width_ref[qf, reach]
        start = offset_ref[qf, b, reach]
        most = min(MAX_WIDTH[min(far, RADIUS)], blocks)
        found = []
        for j in range(most):
            if most == blocks:
                inside = lax.rem(j - start + blocks, blocks) < span
                if far == 0:
                    inside = inside | ((distance == 0) & (b == j))
                found.append((refs, j, present & inside))
            else:
                inside = None if most == 1 and far * 1 <= RADIUS - 2 * (group - 1) else present & (j < span)
                found.append((refs, lax.rem(start + j, blocks), inside))
        return found

    def gather(found, head, column):
        parts = []
        for ref, block, _ in found:
            if isinstance(block, int):
                at = pl.ds(block * BLK, BLK)
            else:
                at = pl.ds(pl.multiple_of(block * BLK, BLK), BLK)
            parts.append(ref[at, column + head * HEAD : column + (head + 1) * HEAD])
        return parts

    def steps(step, base, mine, q_refs, other, chunk, begin):
        far = max(0, step * group - (group - 1))
        most = min(MAX_WIDTH[min(far, RADIUS)], blocks)
        for member in range(group):
            qf = frame_of(mine, place, group, member)
            order = [member] + [i for i in range(group) if i != member]
            batches = [[i] for i in order] if most == blocks else [order]
            for index, batch in enumerate(batches):
                for head in range(heads):
                    for b in range(blocks):
                        found = []
                        for i in batch:
                            kf = frame_of(other, place, group, i)
                            found += pair_slots(b, qf, kf, far, chunk[i])
                        key_slots = jnp.concatenate(gather(found, head, 0), axis=0)
                        value_slots = jnp.concatenate(
                            [
                                jnp.concatenate([v, ones], axis=1)
                                for v in gather(found, head, width)
                            ],
                            axis=0,
                        )
                        low = base + member * tokens + b * BLK
                        rows = slice(low, low + BLK)
                        query = q_refs[member][
                            b * BLK : (b + 1) * BLK, head * HEAD : (head + 1) * HEAD
                        ]
                        oks = [ok for _, _, ok in found]
                        update(
                            rows, query, key_slots, value_slots, oks,
                            m_ref, acc_ref, head, begin and index == 0,
                        )

    for q, k, step, begin in jobs:
        mine, there = unit_at(queries[q], unit, units)
        other, counts = unit_at(keys[k], unit, units)
        guard = counts if there is None else there
        run = functools.partial(
            steps, step, q * group * tokens, mine, q_sets[q], other, chunks[k], begin
        )
        if guard is None:
            run()
        else:
            pl.when(guard)(run)

    def finish():
        for q, spec in enumerate(queries):
            base = q * group * tokens
            slab = 0
            if len(queries) > 1:
                slab = lax.rem(unit_at(spec, unit, units)[0], 2) * group * tokens
            for member in range(group):
                start = slab + (place if member == 0 else group - 1 - place) * tokens
                for head in range(heads):
                    for b in range(blocks):
                        low = base + member * tokens + b * BLK
                        both = acc_ref[head, low : low + BLK, :]
                        at = pl.ds(pl.multiple_of(start + b * BLK, BLK), BLK)
                        out_ref[at, head * HEAD : (head + 1) * HEAD] = (
                            both[:, :HEAD] / both[:, HEAD:]
                        ).astype(out_ref.dtype)

    if ends:
        inner = unit_at(queries[0], unit, units)[1]
        if inner is None:
            finish()
        else:
            pl.when(inner)(finish)


def attend(cfg, bands, queries, chunks, state):
    group, heads, _, query_units, _, jobs, begins, ends = cfg
    tokens = queries[0].shape[0]
    rows = len(query_units) * group * tokens
    m_shape = pltpu.VMEM((heads, rows, BLK), jnp.float32)
    acc_shape = pltpu.VMEM((heads, rows, 2 * HEAD), jnp.float32)
    flat = [in_vmem(c) for pair in chunks for c in pair]
    inputs = [*bands, *[in_vmem(q) for q in queries], *flat, *state]
    outs = [m_shape, acc_shape]
    aliases = {}
    if not begins:
        aliases = {len(inputs) - 2: 0, len(inputs) - 1: 1}
    if ends:
        outs = [jax.ShapeDtypeStruct((rows, heads * HEAD), queries[0].dtype), m_shape, acc_shape]
        aliases = {index: out + 1 for index, out in aliases.items()}
    work = 4 * len(jobs) * (group * tokens) ** 2 * heads * HEAD
    return pl.pallas_call(
        functools.partial(attend_kernel, cfg),
        out_shape=outs,
        in_specs=[SMEM] * 2 + [VMEM] * (len(inputs) - 2),
        out_specs=[VMEM] * len(outs),
        input_output_aliases=aliases,
        compiler_params=params(),
        cost_estimate=pl.CostEstimate(flops=work, bytes_accessed=1 << 20, transcendentals=0),
        name="attend",
    )(*inputs)


def project_kernel(group, ranks, slabs, rows_ref, *refs):
    weights, out_ref = refs[:-1], refs[-1]
    me = lax.axis_index("head")
    base = 0
    if slabs > 1:
        pair = lax.axis_index("frame") // (slabs * group)
        base = (1 - pair) * group * ranks
    total = None
    for offset, weight in enumerate(weights):
        owner = me ^ offset
        left = jnp.concatenate([rows_ref[base + i * ranks + owner] for i in range(group)], axis=1)
        term = jnp.dot(left, weight[...], preferred_element_type=jnp.float32)
        total = term if total is None else total + term
    out_ref[...] = total.astype(out_ref.dtype)


def project(rows, weights, group, slabs):
    ranks = len(weights)
    tokens, columns = rows.shape[1], weights[0].shape[1]
    return pl.pallas_call(
        functools.partial(project_kernel, group, ranks, slabs),
        out_shape=jax.ShapeDtypeStruct((tokens, columns), rows.dtype),
        in_specs=[VMEM] * (1 + ranks),
        out_specs=VMEM,
        compiler_params=params(),
        cost_estimate=pl.CostEstimate(
            flops=2 * rows.size * columns, bytes_accessed=1 << 20, transcendentals=0
        ),
        name="project",
    )(in_vmem(rows), *[in_vmem(w) for w in weights])


def plan(shape, columns):
    frames, local_heads = shape["frame"], columns // HEAD
    group = 2 if local_heads % 2 == 0 and frames % 2 == 0 else 1
    units = frames // group
    return group, units, min(units - 1, (RADIUS + group - 1) // group)


def folds(units, furthest):
    return units == 4 and furthest == units - 1


def edges(units, k, parity):
    sends = []
    for low in range(parity, units - 1, 2):
        if low + 1 - k >= 0:
            sends.append((low, low + 1))
        if low + k < units:
            sends.append((low + 1, low))
    return sends


def on_device(queries, keys, values, band_width, band_offset, out_weight):
    frames, ranks = lax.axis_size("frame"), lax.axis_size("head")
    tokens = queries.shape[0]
    group, units, furthest = plan({"frame": frames}, queries.shape[1])
    heads = queries.shape[1] // HEAD // group

    def along(value, steps):
        pairs = [(a * group + i, b * group + i) for a, b in steps for i in range(group)]
        return lax.ppermute(value, "frame", pairs)

    bands = (band_width, jnp.transpose(band_offset, (0, 2, 1)))
    *pieces, band_width, band_offset = split(queries, keys, values, bands, group)
    bands = (band_width, band_offset)
    chunks, query_rows = [pieces[0]], [pieces[1]]
    if group == 2:
        swap = [(f, f ^ 1) for f in range(frames)]
        chunks.append(lax.ppermute(pieces[2], "frame", swap))
        query_rows.append(lax.ppermute(pieces[3], "frame", swap))

    weights = {0: out_weight}
    bit = ranks // 2
    while bit:
        for offset in list(weights):
            pairs = [(h, h ^ bit) for h in range(ranks)]
            weights[offset ^ bit] = lax.ppermute(weights[offset], "head", pairs)
        bit //= 2
    weights = [weights[o] for o in range(ranks)]

    own = ("own", 0, 0)
    fold = folds(units, furthest)
    if fold:
        outer = [(0, 1), (3, 2)]
        inner = [(1, 2), (2, 1)]
        near = [along(c, inner) for c in chunks]
        behind = [along(c, outer) for c in chunks]
        theirs = [along(q, outer) for q in query_rows]
        distant = [along(c, inner) for c in behind]
        queries = tuple(("fold", n, 0) for n in (0, -1))
        rows = query_rows + theirs
        calls = [
            ([(0, chunks)], [(0, 0, 0, True)]),
            ([(1, near)], [(0, 0, 1, False)]),
            (
                [(-1, behind), (0, chunks), (1, near)],
                [(1, 0, 0, True), (1, 1, 1, False), (0, 0, 1, False), (1, 2, 2, False)],
            ),
            ([(2, distant)], [(1, 0, 3, False), (0, 0, 2, False)]),
        ]
        state = []
        for index, (held, jobs) in enumerate(calls):
            keys = tuple(("fold", n, 0) for n, _ in held)
            used = {q for q, _, _, _ in jobs}
            given = rows if 1 in used else query_rows + query_rows
            cfg = (group, heads, units, queries, keys, tuple(jobs), index == 0, index == len(calls) - 1)
            state = attend(cfg, bands, given, [c for _, c in held], state)
    else:
        held, arrived = [chunks, chunks], []
        for k in range(1, furthest + 1):
            held = [
                [along(c, edges(units, k, parity)) for c in source]
                for parity, source in enumerate(reversed(held))
                if edges(units, k, parity)
            ]
            arrived.append(held)
        cfg = (group, heads, units, (own,), (own,), ((0, 0, 0, True),), True, False)
        state = attend(cfg, bands, query_rows, [chunks], [])
        for k, received in enumerate(arrived, 1):
            keys = tuple(("edge", k, parity) for parity in range(2) if edges(units, k, parity))
            jobs = tuple((0, i, k, False) for i in range(len(keys)))
            cfg = (group, heads, units, (own,), keys, jobs, False, k == furthest)
            state = attend(cfg, bands, query_rows, received, state)
    attended = state[0]

    slabs = 2 if fold else 1
    members = [
        [(f * ranks + h) for f in range(u * group, (u + slabs) * group) for h in range(ranks)]
        for u in range(0, units, slabs)
    ]
    blocks = attended.reshape(slabs * group * ranks, tokens // ranks, heads * HEAD)
    rows = lax.all_to_all(
        blocks, ("frame", "head"), split_axis=0, concat_axis=0, tiled=True,
        axis_index_groups=members,
    )
    return project(rows, weights, group, slabs)


def solution(mesh):
    placed = (P("frame", "head"), P("frame", "head"), P("frame", "head"), P(), P(), P("head", None))
    return jax.shard_map(
        on_device, mesh=mesh, in_specs=placed, out_specs=P(("frame", "head"), None), check_vma=False
    )
```

```python
import functools
import math

import jax
import jax.numpy as jnp
from jax import lax
from jax.experimental import pallas as pl
from jax.experimental.pallas import tpu as pltpu
from jax.sharding import PartitionSpec as P


HEAD = 128
BLK = 128
RADIUS = 7
MAX_WIDTH = (4, 4, 2, 2, 1, 1, 1, 1)
MASKED = -1e30
EXPONENT = math.log2(math.e) / math.sqrt(HEAD)

VMEM = pl.BlockSpec(memory_space=pltpu.VMEM)
SMEM = pl.BlockSpec(memory_space=pltpu.SMEM)
HBM = pl.BlockSpec(memory_space=pltpu.HBM)


def in_vmem(value):
    return pltpu.with_memory_space_constraint(value, pltpu.VMEM)


def in_hbm(value):
    return pltpu.with_memory_space_constraint(value, pltpu.HBM)


def params():
    return pltpu.CompilerParams(vmem_limit_bytes=32 << 20)


def split_kernel(group, q_ref, k_ref, v_ref, width_ref, offset_ref, *refs):
    outs, sem = refs[:-1], refs[-1]
    width = outs[0].shape[1] // 2
    place = lax.rem(lax.axis_index("frame"), group)
    copies = []
    for part in range(group):
        column = (place if part == 0 else 1 - place) * width
        columns = pl.ds(pl.multiple_of(column, HEAD), width)
        pair, rows = outs[2 * part], outs[2 * part + 1]
        for source, target in (
            (k_ref, pair.at[:, :width]),
            (v_ref, pair.at[:, width:]),
            (q_ref, rows),
        ):
            copies.append(
                pltpu.make_async_copy(source.at[:, columns], target, sem.at[len(copies)])
            )
    for source, target in ((width_ref, outs[-2]), (offset_ref, outs[-1])):
        copies.append(pltpu.make_async_copy(source, target, sem.at[len(copies)]))
    for copy in copies:
        copy.start()
    for copy in copies:
        copy.wait()


def split(queries, keys, values, bands, group):
    tokens, columns = queries.shape
    width = columns // group
    pair = pltpu.VMEM((tokens, 2 * width), queries.dtype)
    rows = pltpu.VMEM((tokens, width), queries.dtype)
    return pl.pallas_call(
        functools.partial(split_kernel, group),
        out_shape=[pair, rows] * group + [pltpu.SMEM(b.shape, b.dtype) for b in bands],
        in_specs=[HBM] * 5,
        out_specs=[VMEM] * (2 * group) + [SMEM] * 2,
        scratch_shapes=[pltpu.SemaphoreType.DMA((3 * group + 2,))],
        compiler_params=params(),
        name="split",
    )(*[in_hbm(v) for v in (queries, keys, values, *bands)])


def frame_of(unit, place, group, member):
    return unit * group + (place if member == 0 else group - 1 - place)


def update(rows, query, key_slots, value_slots, oks, m_ref, acc_ref, head, first):
    scores = lax.dot_general(
        query, key_slots, (((1,), (1,)), ((), ())), preferred_element_type=jnp.float32
    )
    pieces = [scores[:, BLK * j : BLK * (j + 1)] for j in range(len(oks))]
    pieces = [s if ok is None else jnp.where(ok, s, MASKED) for s, ok in zip(pieces, oks)]
    tallest = functools.reduce(jnp.maximum, pieces)
    tallest = jnp.max(tallest, axis=1, keepdims=True)
    if first:
        peak = jnp.broadcast_to(tallest, (BLK, BLK))
    else:
        before = m_ref[head, rows, :]
        peak = jnp.maximum(before, tallest)
    weights = [jnp.exp2((s - peak) * EXPONENT).astype(jnp.bfloat16) for s in pieces]
    weights = jnp.concatenate(weights, axis=1)
    added = jnp.dot(weights, value_slots, preferred_element_type=jnp.float32)
    if not first:
        rescale = jnp.exp2((before - peak) * EXPONENT)
        rescale = jnp.concatenate([rescale, rescale], axis=1)
        added = acc_ref[head, rows, :] * rescale + added
    acc_ref[head, rows, :] = added
    m_ref[head, rows, :] = peak


def unit_at(spec, unit, units):
    kind, step, parity = spec
    if kind == "own":
        return unit, None
    if kind == "edge":
        facing = 1 - 2 * lax.rem(unit, 2)
        other = unit + step * (facing if parity == 0 else -facing)
        return other, (other >= 0) & (other < units)
    inwards = jnp.where(2 * unit < units, 1, -1)
    return unit + step * inwards, (unit > 0) & (unit < units - 1)


def attend_kernel(cfg, width_ref, offset_ref, *refs):
    group, heads, units, queries, keys, jobs, begins, ends = cfg
    q_sets = [refs[group * i : group * (i + 1)] for i in range(len(queries))]
    refs = refs[group * len(queries) :]
    chunks = [refs[group * i : group * (i + 1)] for i in range(len(keys))]
    refs = refs[group * len(keys) :]
    if not begins:
        refs = refs[2:]
    if ends:
        out_ref, m_ref, acc_ref = refs
    else:
        m_ref, acc_ref = refs
    tokens = q_sets[0][0].shape[0]
    blocks = tokens // BLK
    width = heads * HEAD
    me = lax.axis_index("frame")
    unit, place = me // group, lax.rem(me, group)
    ones = jnp.ones((BLK, HEAD), jnp.bfloat16)

    def pair_slots(b, qf, kf, far, refs):
        distance = jnp.abs(qf - kf)
        present = distance <= RADIUS
        reach = jnp.minimum(distance, RADIUS)
        span = width_ref[qf, reach]
        start = offset_ref[qf, b, reach]
        most = min(MAX_WIDTH[min(far, RADIUS)], blocks)
        found = []
        for j in range(most):
            if most == blocks:
                inside = lax.rem(j - start + blocks, blocks) < span
                if far == 0:
                    inside = inside | ((distance == 0) & (b == j))
                found.append((refs, j, present & inside))
            else:
                inside = None if most == 1 and far * 1 <= RADIUS - 2 * (group - 1) else present & (j < span)
                found.append((refs, lax.rem(start + j, blocks), inside))
        return found

    def gather(found, head, column):
        parts = []
        for ref, block, _ in found:
            if isinstance(block, int):
                at = pl.ds(block * BLK, BLK)
            else:
                at = pl.ds(pl.multiple_of(block * BLK, BLK), BLK)
            parts.append(ref[at, column + head * HEAD : column + (head + 1) * HEAD])
        return parts

    def steps(step, base, mine, q_refs, other, chunk, begin):
        far = max(0, step * group - (group - 1))
        most = min(MAX_WIDTH[min(far, RADIUS)], blocks)
        for member in range(group):
            qf = frame_of(mine, place, group, member)
            order = [member] + [i for i in range(group) if i != member]
            batches = [[i] for i in order] if most == blocks else [order]
            for index, batch in enumerate(batches):
                for head in range(heads):
                    for b in range(blocks):
                        found = []
                        for i in batch:
                            kf = frame_of(other, place, group, i)
                            found += pair_slots(b, qf, kf, far, chunk[i])
                        key_slots = jnp.concatenate(gather(found, head, 0), axis=0)
                        value_slots = jnp.concatenate(
                            [
                                jnp.concatenate([v, ones], axis=1)
                                for v in gather(found, head, width)
                            ],
                            axis=0,
                        )
                        low = base + member * tokens + b * BLK
                        rows = slice(low, low + BLK)
                        query = q_refs[member][
                            b * BLK : (b + 1) * BLK, head * HEAD : (head + 1) * HEAD
                        ]
                        oks = [ok for _, _, ok in found]
                        update(
                            rows, query, key_slots, value_slots, oks,
                            m_ref, acc_ref, head, begin and index == 0,
                        )

    for q, k, step, begin in jobs:
        mine, there = unit_at(queries[q], unit, units)
        other, counts = unit_at(keys[k], unit, units)
        guard = counts if there is None else there
        run = functools.partial(
            steps, step, q * group * tokens, mine, q_sets[q], other, chunks[k], begin
        )
        if guard is None:
            run()
        else:
            pl.when(guard)(run)

    def finish():
        for q, spec in enumerate(queries):
            base = q * group * tokens
            slab = 0
            if len(queries) > 1:
                slab = lax.rem(unit_at(spec, unit, units)[0], 2) * group * tokens
            for member in range(group):
                start = slab + (place if member == 0 else group - 1 - place) * tokens
                for head in range(heads):
                    for b in range(blocks):
                        low = base + member * tokens + b * BLK
                        both = acc_ref[head, low : low + BLK, :]
                        at = pl.ds(pl.multiple_of(start + b * BLK, BLK), BLK)
                        out_ref[at, head * HEAD : (head + 1) * HEAD] = (
                            both[:, :HEAD] / both[:, HEAD:]
                        ).astype(out_ref.dtype)

    if ends:
        inner = unit_at(queries[0], unit, units)[1]
        if inner is None:
            finish()
        else:
            pl.when(inner)(finish)


def attend(cfg, bands, queries, chunks, state):
    group, heads, _, query_units, _, jobs, begins, ends = cfg
    tokens = queries[0].shape[0]
    rows = len(query_units) * group * tokens
    m_shape = pltpu.VMEM((heads, rows, BLK), jnp.float32)
    acc_shape = pltpu.VMEM((heads, rows, 2 * HEAD), jnp.float32)
    flat = [in_vmem(c) for pair in chunks for c in pair]
    inputs = [*bands, *[in_vmem(q) for q in queries], *flat, *state]
    outs = [m_shape, acc_shape]
    aliases = {}
    if not begins:
        aliases = {len(inputs) - 2: 0, len(inputs) - 1: 1}
    if ends:
        outs = [jax.ShapeDtypeStruct((rows, heads * HEAD), queries[0].dtype), m_shape, acc_shape]
        aliases = {index: out + 1 for index, out in aliases.items()}
    work = 4 * len(jobs) * (group * tokens) ** 2 * heads * HEAD
    return pl.pallas_call(
        functools.partial(attend_kernel, cfg),
        out_shape=outs,
        in_specs=[SMEM] * 2 + [VMEM] * (len(inputs) - 2),
        out_specs=[VMEM] * len(outs),
        input_output_aliases=aliases,
        compiler_params=params(),
        cost_estimate=pl.CostEstimate(flops=work, bytes_accessed=1 << 20, transcendentals=0),
        name="attend",
    )(*inputs)


def project_kernel(group, ranks, slabs, rows_ref, *refs):
    weights, (out_ref, kept, sem) = refs[: ranks], refs[ranks:]
    copy = pltpu.make_async_copy(weights[0], kept, sem)
    copy.start()
    me = lax.axis_index("head")
    base = 0
    if slabs > 1:
        pair = lax.axis_index("frame") // (slabs * group)
        base = (1 - pair) * group * ranks
    total = None
    for offset in [*range(1, ranks), 0]:
        weight = weights[offset]
        if offset == 0:
            copy.wait()
            weight = kept
        owner = me ^ offset
        left = jnp.concatenate([rows_ref[base + i * ranks + owner] for i in range(group)], axis=1)
        term = jnp.dot(left, weight[...], preferred_element_type=jnp.float32)
        total = term if total is None else total + term
    out_ref[...] = total.astype(out_ref.dtype)


def project(rows, weights, group, slabs):
    ranks = len(weights)
    tokens, columns = rows.shape[1], weights[0].shape[1]
    return pl.pallas_call(
        functools.partial(project_kernel, group, ranks, slabs),
        out_shape=jax.ShapeDtypeStruct((tokens, columns), rows.dtype),
        in_specs=[VMEM, HBM] + [VMEM] * (ranks - 1),
        out_specs=VMEM,
        scratch_shapes=[pltpu.VMEM(weights[0].shape, rows.dtype), pltpu.SemaphoreType.DMA],
        compiler_params=params(),
        cost_estimate=pl.CostEstimate(
            flops=2 * rows.size * columns, bytes_accessed=1 << 20, transcendentals=0
        ),
        name="project",
    )(in_vmem(rows), in_hbm(weights[0]), *[in_vmem(w) for w in weights[1:]])


def plan(shape, columns):
    frames, local_heads = shape["frame"], columns // HEAD
    group = 2 if local_heads % 2 == 0 and frames % 2 == 0 else 1
    units = frames // group
    return group, units, min(units - 1, (RADIUS + group - 1) // group)


def folds(units, furthest):
    return units == 4 and furthest == units - 1


def edges(units, k, parity):
    sends = []
    for low in range(parity, units - 1, 2):
        if low + 1 - k >= 0:
            sends.append((low, low + 1))
        if low + k < units:
            sends.append((low + 1, low))
    return sends


def on_device(queries, keys, values, band_width, band_offset, out_weight):
    frames, ranks = lax.axis_size("frame"), lax.axis_size("head")
    tokens = queries.shape[0]
    group, units, furthest = plan({"frame": frames}, queries.shape[1])
    heads = queries.shape[1] // HEAD // group

    def along(value, steps):
        pairs = [(a * group + i, b * group + i) for a, b in steps for i in range(group)]
        return lax.ppermute(value, "frame", pairs)

    bands = (band_width, jnp.transpose(band_offset, (0, 2, 1)))
    *pieces, band_width, band_offset = split(queries, keys, values, bands, group)
    bands = (band_width, band_offset)
    chunks, query_rows = [pieces[0]], [pieces[1]]
    if group == 2:
        swap = [(f, f ^ 1) for f in range(frames)]
        chunks.append(lax.ppermute(pieces[2], "frame", swap))
        query_rows.append(lax.ppermute(pieces[3], "frame", swap))

    weights = {0: out_weight}
    bit = ranks // 2
    while bit:
        for offset in list(weights):
            pairs = [(h, h ^ bit) for h in range(ranks)]
            weights[offset ^ bit] = lax.ppermute(weights[offset], "head", pairs)
        bit //= 2
    weights = [weights[o] for o in range(ranks)]

    own = ("own", 0, 0)
    fold = folds(units, furthest)
    if fold:
        outer = [(0, 1), (3, 2)]
        inner = [(1, 2), (2, 1)]
        near = [along(c, inner) for c in chunks]
        behind = [along(c, outer) for c in chunks]
        theirs = [along(q, outer) for q in query_rows]
        distant = [along(c, inner) for c in behind]
        queries = tuple(("fold", n, 0) for n in (0, -1))
        rows = query_rows + theirs
        calls = [
            ([(0, chunks)], [(0, 0, 0, True)]),
            ([(1, near)], [(0, 0, 1, False)]),
            (
                [(-1, behind), (0, chunks), (1, near)],
                [(1, 0, 0, True), (1, 1, 1, False), (0, 0, 1, False), (1, 2, 2, False)],
            ),
            ([(2, distant)], [(1, 0, 3, False), (0, 0, 2, False)]),
        ]
        state = []
        for index, (held, jobs) in enumerate(calls):
            keys = tuple(("fold", n, 0) for n, _ in held)
            used = {q for q, _, _, _ in jobs}
            given = rows if 1 in used else query_rows + query_rows
            cfg = (group, heads, units, queries, keys, tuple(jobs), index == 0, index == len(calls) - 1)
            state = attend(cfg, bands, given, [c for _, c in held], state)
    else:
        held, arrived = [chunks, chunks], []
        for k in range(1, furthest + 1):
            held = [
                [along(c, edges(units, k, parity)) for c in source]
                for parity, source in enumerate(reversed(held))
                if edges(units, k, parity)
            ]
            arrived.append(held)
        cfg = (group, heads, units, (own,), (own,), ((0, 0, 0, True),), True, False)
        state = attend(cfg, bands, query_rows, [chunks], [])
        for k, received in enumerate(arrived, 1):
            keys = tuple(("edge", k, parity) for parity in range(2) if edges(units, k, parity))
            jobs = tuple((0, i, k, False) for i in range(len(keys)))
            cfg = (group, heads, units, (own,), keys, jobs, False, k == furthest)
            state = attend(cfg, bands, query_rows, received, state)
    attended = state[0]

    slabs = 2 if fold else 1
    members = [
        [(f * ranks + h) for f in range(u * group, (u + slabs) * group) for h in range(ranks)]
        for u in range(0, units, slabs)
    ]
    blocks = attended.reshape(slabs * group * ranks, tokens // ranks, heads * HEAD)
    rows = lax.all_to_all(
        blocks, ("frame", "head"), split_axis=0, concat_axis=0, tiled=True,
        axis_index_groups=members,
    )
    return project(rows, weights, group, slabs)


def solution(mesh):
    placed = (P("frame", "head"), P("frame", "head"), P("frame", "head"), P(), P(), P("head", None))
    return jax.shard_map(
        on_device, mesh=mesh, in_specs=placed, out_specs=P(("frame", "head"), None), check_vma=False
    )
```

```python
import functools
import math

import jax
import jax.numpy as jnp
from jax import lax
from jax.experimental import pallas as pl
from jax.experimental.pallas import tpu as pltpu
from jax.sharding import PartitionSpec as P


HEAD = 128
BLK = 128
RADIUS = 7
MAX_WIDTH = (4, 4, 2, 2, 1, 1, 1, 1)
MASKED = -1e30
EXPONENT = math.log2(math.e) / math.sqrt(HEAD)

VMEM = pl.BlockSpec(memory_space=pltpu.VMEM)
SMEM = pl.BlockSpec(memory_space=pltpu.SMEM)
HBM = pl.BlockSpec(memory_space=pltpu.HBM)


def in_vmem(value):
    return pltpu.with_memory_space_constraint(value, pltpu.VMEM)


def in_hbm(value):
    return pltpu.with_memory_space_constraint(value, pltpu.HBM)


def params():
    return pltpu.CompilerParams(vmem_limit_bytes=32 << 20)


def split_kernel(group, q_ref, k_ref, v_ref, width_ref, offset_ref, *refs):
    outs, sem = refs[:-1], refs[-1]
    width = outs[0].shape[1] // 2
    place = lax.rem(lax.axis_index("frame"), group)
    copies = []
    for part in range(group):
        column = (place if part == 0 else 1 - place) * width
        columns = pl.ds(pl.multiple_of(column, HEAD), width)
        pair, rows = outs[2 * part], outs[2 * part + 1]
        for source, target in (
            (k_ref, pair.at[:, :width]),
            (v_ref, pair.at[:, width:]),
            (q_ref, rows),
        ):
            copies.append(
                pltpu.make_async_copy(source.at[:, columns], target, sem.at[len(copies)])
            )
    for source, target in ((width_ref, outs[-2]), (offset_ref, outs[-1])):
        copies.append(pltpu.make_async_copy(source, target, sem.at[len(copies)]))
    for copy in copies:
        copy.start()
    for copy in copies:
        copy.wait()


def split(queries, keys, values, bands, group):
    tokens, columns = queries.shape
    width = columns // group
    pair = pltpu.VMEM((tokens, 2 * width), queries.dtype)
    rows = pltpu.VMEM((tokens, width), queries.dtype)
    return pl.pallas_call(
        functools.partial(split_kernel, group),
        out_shape=[pair, rows] * group + [pltpu.SMEM(b.shape, b.dtype) for b in bands],
        in_specs=[HBM] * 5,
        out_specs=[VMEM] * (2 * group) + [SMEM] * 2,
        scratch_shapes=[pltpu.SemaphoreType.DMA((3 * group + 2,))],
        compiler_params=params(),
        name="split",
    )(*[in_hbm(v) for v in (queries, keys, values, *bands)])


def frame_of(unit, place, group, member):
    return unit * group + (place if member == 0 else group - 1 - place)


def update(rows, query, key_slots, value_slots, oks, m_ref, acc_ref, head, first):
    scores = lax.dot_general(
        query, key_slots, (((1,), (1,)), ((), ())), preferred_element_type=jnp.float32
    )
    pieces = [scores[:, BLK * j : BLK * (j + 1)] for j in range(len(oks))]
    pieces = [s if ok is None else jnp.where(ok, s, MASKED) for s, ok in zip(pieces, oks)]
    tallest = functools.reduce(jnp.maximum, pieces)
    tallest = jnp.max(tallest, axis=1, keepdims=True)
    if first:
        peak = jnp.broadcast_to(tallest, (BLK, BLK))
    else:
        before = m_ref[head, rows, :]
        peak = jnp.maximum(before, tallest)
    weights = [jnp.exp2((s - peak) * EXPONENT).astype(jnp.bfloat16) for s in pieces]
    weights = jnp.concatenate(weights, axis=1)
    added = jnp.dot(weights, value_slots, preferred_element_type=jnp.float32)
    if not first:
        rescale = jnp.exp2((before - peak) * EXPONENT)
        rescale = jnp.concatenate([rescale, rescale], axis=1)
        added = acc_ref[head, rows, :] * rescale + added
    acc_ref[head, rows, :] = added
    m_ref[head, rows, :] = peak


def attend_kernel(cfg, width_ref, offset_ref, *refs):
    group, heads, shifts, units, begins, ends = cfg
    q_refs, refs = refs[:group], refs[group:]
    chunks = [refs[group * i : group * (i + 1)] for i in range(len(shifts))]
    refs = refs[group * len(shifts) :]
    if not begins:
        refs = refs[2:]
    if ends:
        keep_ref, give_ref, m_ref, acc_ref = refs
    else:
        m_ref, acc_ref = refs
    tokens = q_refs[0].shape[0]
    blocks = tokens // BLK
    width = heads * HEAD
    me = lax.axis_index("frame")
    unit, place = me // group, lax.rem(me, group)
    ones = jnp.ones((BLK, HEAD), jnp.bfloat16)

    def pair_slots(b, qf, kf, far, refs):
        distance = jnp.abs(qf - kf)
        present = distance <= RADIUS
        reach = jnp.minimum(distance, RADIUS)
        span = width_ref[qf, reach]
        start = offset_ref[qf, b, reach]
        most = min(MAX_WIDTH[min(far, RADIUS)], blocks)
        found = []
        for j in range(most):
            if most == blocks:
                inside = lax.rem(j - start + blocks, blocks) < span
                if far == 0:
                    inside = inside | ((distance == 0) & (b == j))
                found.append((refs, j, present & inside))
            else:
                inside = None if most == 1 and far * 1 <= RADIUS - 2 * (group - 1) else present & (j < span)
                found.append((refs, lax.rem(start + j, blocks), inside))
        return found

    def gather(found, head, column):
        parts = []
        for ref, block, _ in found:
            if isinstance(block, int):
                at = pl.ds(block * BLK, BLK)
            else:
                at = pl.ds(pl.multiple_of(block * BLK, BLK), BLK)
            parts.append(ref[at, column + head * HEAD : column + (head + 1) * HEAD])
        return parts

    def steps(step, other, chunk, begin):
        far = max(0, step * group - (group - 1))
        most = min(MAX_WIDTH[min(far, RADIUS)], blocks)
        for member in range(group):
            qf = frame_of(unit, place, group, member)
            order = [member] + [i for i in range(group) if i != member]
            batches = [[i] for i in order] if most == blocks else [order]
            for index, batch in enumerate(batches):
                for head in range(heads):
                    for b in range(blocks):
                        found = []
                        for i in batch:
                            kf = frame_of(other, place, group, i)
                            found += pair_slots(b, qf, kf, far, chunk[i])
                        key_slots = jnp.concatenate(gather(found, head, 0), axis=0)
                        value_slots = jnp.concatenate(
                            [
                                jnp.concatenate([v, ones], axis=1)
                                for v in gather(found, head, width)
                            ],
                            axis=0,
                        )
                        rows = slice(member * tokens + b * BLK, member * tokens + (b + 1) * BLK)
                        query = q_refs[member][
                            b * BLK : (b + 1) * BLK, head * HEAD : (head + 1) * HEAD
                        ]
                        oks = [ok for _, _, ok in found]
                        update(
                            rows, query, key_slots, value_slots, oks,
                            m_ref, acc_ref, head, begin and index == 0,
                        )

    facing = 1 - 2 * lax.rem(unit, 2)
    for (step, parity), chunk in zip(shifts, chunks):
        if step == 0:
            steps(0, unit, chunk, begins)
        else:
            other = unit + step * (facing if parity == 0 else -facing)

            @pl.when((other >= 0) & (other < units))
            def _(step=step, other=other, chunk=chunk):
                steps(step, other, chunk, False)

    if ends:
        halves, rank_rows = keep_ref.shape[0] // group, keep_ref.shape[1]
        rank = lax.axis_index("head")
        for head in range(heads):
            columns = slice(head * HEAD, (head + 1) * HEAD)
            for r in range(keep_ref.shape[0]):
                for ref, low in ((keep_ref, 0), (give_ref, 1)):
                    block = rank ^ (2 * (r % halves) + low)
                    start = (r // halves) * tokens + block * rank_rows
                    at = pl.ds(pl.multiple_of(start, rank_rows), rank_rows)
                    both = acc_ref[head, at, :]
                    ref[r, :, columns] = (both[:, :HEAD] / both[:, HEAD:]).astype(ref.dtype)


def attend(cfg, bands, queries, chunks, state):
    group, heads, _, _, begins, ends = cfg
    tokens = queries[0].shape[0]
    rows = group * tokens
    m_shape = pltpu.VMEM((heads, rows, BLK), jnp.float32)
    acc_shape = pltpu.VMEM((heads, rows, 2 * HEAD), jnp.float32)
    flat = [in_vmem(c) for pair in chunks for c in pair]
    inputs = [*bands, *[in_vmem(q) for q in queries], *flat, *state]
    outs = [m_shape, acc_shape]
    aliases = {}
    if not begins:
        aliases = {len(inputs) - 2: 0, len(inputs) - 1: 1}
    if ends:
        sent = group * lax.axis_size("head") // 2
        part = pltpu.VMEM((sent, rows // (2 * sent), heads * HEAD), queries[0].dtype)
        outs = [part, part, m_shape, acc_shape]
        aliases = {index: out + 2 for index, out in aliases.items()}
    work = 4 * len(flat) * tokens * rows * heads * HEAD
    return pl.pallas_call(
        functools.partial(attend_kernel, cfg),
        out_shape=outs,
        in_specs=[SMEM] * 2 + [VMEM] * (len(inputs) - 2),
        out_specs=[VMEM] * len(outs),
        input_output_aliases=aliases,
        compiler_params=params(),
        cost_estimate=pl.CostEstimate(flops=work, bytes_accessed=1 << 20, transcendentals=0),
    )(*inputs)


def pack_kernel(keep_ref, got_ref, *outs):
    for r, out in enumerate(outs):
        out[0] = keep_ref[r]
        out[1] = got_ref[r]


def pack(keep, got):
    count, *shape = keep.shape
    return pl.pallas_call(
        pack_kernel,
        out_shape=[pltpu.VMEM((2, *shape), keep.dtype)] * count,
        in_specs=[VMEM] * 2,
        out_specs=[VMEM] * count,
        compiler_params=params(),
        name="pack",
    )(in_vmem(keep), in_vmem(got))


def project_kernel(group, ranks, *refs):
    rows, weights, out_ref = refs[: group * ranks // 2], refs[group * ranks // 2 : -1], refs[-1]
    place = lax.rem(lax.axis_index("frame"), group)
    total = None
    for offset, weight in enumerate(weights):
        parts = [rows[i * ranks // 2 + offset // 2][offset % 2] for i in range(group)]
        left = jnp.concatenate(parts, axis=1)
        if group == 2:
            left = jnp.where(place == 0, left, jnp.concatenate(parts[::-1], axis=1))
        term = jnp.dot(left, weight[...], preferred_element_type=jnp.float32)
        total = term if total is None else total + term
    out_ref[...] = total.astype(out_ref.dtype)


def project(rows, weights, group):
    ranks = len(weights)
    tokens, columns = rows[0].shape[1], weights[0].shape[1]
    return pl.pallas_call(
        functools.partial(project_kernel, group, ranks),
        out_shape=jax.ShapeDtypeStruct((tokens, columns), rows[0].dtype),
        in_specs=[VMEM] * (len(rows) + ranks),
        out_specs=VMEM,
        compiler_params=params(),
        cost_estimate=pl.CostEstimate(
            flops=4 * rows[0].size * len(rows) * columns, bytes_accessed=1 << 20, transcendentals=0
        ),
        name="project",
    )(*[in_vmem(r) for r in rows], *[in_vmem(w) for w in weights])


def plan(shape, columns):
    frames, local_heads = shape["frame"], columns // HEAD
    group = 2 if local_heads % 2 == 0 and frames % 2 == 0 else 1
    units = frames // group
    return group, units, min(units - 1, (RADIUS + group - 1) // group)


def edges(units, k, parity):
    sends = []
    for low in range(parity, units - 1, 2):
        if low + 1 - k >= 0:
            sends.append((low, low + 1))
        if low + k < units:
            sends.append((low + 1, low))
    return sends


def on_device(queries, keys, values, band_width, band_offset, out_weight):
    frames, ranks = lax.axis_size("frame"), lax.axis_size("head")
    group, units, furthest = plan({"frame": frames}, queries.shape[1])
    heads = queries.shape[1] // HEAD // group

    def along(value, steps):
        pairs = [(a * group + i, b * group + i) for a, b in steps for i in range(group)]
        return lax.ppermute(value, "frame", pairs)

    bands = (band_width, jnp.transpose(band_offset, (0, 2, 1)))
    *pieces, band_width, band_offset = split(queries, keys, values, bands, group)
    bands = (band_width, band_offset)
    chunks, query_rows = [pieces[0]], [pieces[1]]
    if group == 2:
        swap = [(f, f ^ 1) for f in range(frames)]
        chunks.append(lax.ppermute(pieces[2], "frame", swap))
        query_rows.append(lax.ppermute(pieces[3], "frame", swap))

    weights = {0: out_weight}
    bit = ranks // 2
    while bit:
        for offset in list(weights):
            pairs = [(h, h ^ bit) for h in range(ranks)]
            weights[offset ^ bit] = lax.ppermute(weights[offset], "head", pairs)
        bit //= 2
    weights = [weights[o] for o in range(ranks)]

    held, arrived = [chunks, chunks], []
    for k in range(1, furthest + 1):
        held = [
            [along(c, edges(units, k, parity)) for c in source]
            for parity, source in enumerate(reversed(held))
            if edges(units, k, parity)
        ]
        arrived.append(held)

    cfg = (group, heads, ((0, 0),), units, True, False)
    state = attend(cfg, bands, query_rows, [chunks], [])
    for k, received in enumerate(arrived, 1):
        shifts = tuple((k, parity) for parity in range(2) if edges(units, k, parity))
        cfg = (group, heads, shifts, units, False, k == furthest)
        state = attend(cfg, bands, query_rows, received, state)
    keep, give = state[:2]
    got = lax.ppermute(give, "head", [(h, h ^ 1) for h in range(ranks)])
    packed = pack(keep, got)
    rows = [packed[0]]
    for r in range(1, len(packed)):
        over, high = r // (ranks // 2), 2 * (r % (ranks // 2))
        pairs = [
            (f * ranks + h, (f ^ over) * ranks + (h ^ high))
            for f in range(frames)
            for h in range(ranks)
        ]
        rows.append(lax.ppermute(packed[r], ("frame", "head"), pairs))
    return project(rows, weights, group)


def solution(mesh):
    placed = (P("frame", "head"), P("frame", "head"), P("frame", "head"), P(), P(), P("head", None))
    return jax.shard_map(
        on_device, mesh=mesh, in_specs=placed, out_specs=P(("frame", "head"), None), check_vma=False
    )
```

```python
import functools
import math

import jax
import jax.numpy as jnp
from jax import lax
from jax.experimental import pallas as pl
from jax.experimental.pallas import tpu as pltpu
from jax.sharding import PartitionSpec as P


HEAD = 128
BLK = 128
RADIUS = 7
MAX_WIDTH = (4, 4, 2, 2, 1, 1, 1, 1)
MASKED = -1e30
PARTS = 3
EXPONENT = math.log2(math.e) / math.sqrt(HEAD)

VMEM = pl.BlockSpec(memory_space=pltpu.VMEM)
SMEM = pl.BlockSpec(memory_space=pltpu.SMEM)
HBM = pl.BlockSpec(memory_space=pltpu.HBM)


def in_vmem(value):
    return pltpu.with_memory_space_constraint(value, pltpu.VMEM)


def in_hbm(value):
    return pltpu.with_memory_space_constraint(value, pltpu.HBM)


def params():
    return pltpu.CompilerParams(vmem_limit_bytes=32 << 20)


def split_kernel(group, q_ref, k_ref, v_ref, width_ref, offset_ref, *refs):
    outs, sem = refs[:-1], refs[-1]
    width = outs[0].shape[1] // 2
    place = lax.rem(lax.axis_index("frame"), group)
    copies = []
    for part in range(group):
        column = (place if part == 0 else 1 - place) * width
        columns = pl.ds(pl.multiple_of(column, HEAD), width)
        pair, rows = outs[2 * part], outs[2 * part + 1]
        for source, target in (
            (k_ref, pair.at[:, :width]),
            (v_ref, pair.at[:, width:]),
            (q_ref, rows),
        ):
            copies.append(
                pltpu.make_async_copy(source.at[:, columns], target, sem.at[len(copies)])
            )
    for source, target in ((width_ref, outs[-2]), (offset_ref, outs[-1])):
        copies.append(pltpu.make_async_copy(source, target, sem.at[len(copies)]))
    for copy in copies:
        copy.start()
    for copy in copies:
        copy.wait()


def split(queries, keys, values, bands, group):
    tokens, columns = queries.shape
    width = columns // group
    pair = pltpu.VMEM((tokens, 2 * width), queries.dtype)
    rows = pltpu.VMEM((tokens, width), queries.dtype)
    return pl.pallas_call(
        functools.partial(split_kernel, group),
        out_shape=[pair, rows] * group + [pltpu.SMEM(b.shape, b.dtype) for b in bands],
        in_specs=[HBM] * 5,
        out_specs=[VMEM] * (2 * group) + [SMEM] * 2,
        scratch_shapes=[pltpu.SemaphoreType.DMA((3 * group + 2,))],
        compiler_params=params(),
        name="split",
    )(*[in_hbm(v) for v in (queries, keys, values, *bands)])


def frame_of(unit, place, group, member):
    return unit * group + (place if member == 0 else group - 1 - place)


def update(rows, query, key_slots, value_slots, oks, m_ref, acc_ref, head, first):
    scores = lax.dot_general(
        query, key_slots, (((1,), (1,)), ((), ())), preferred_element_type=jnp.float32
    )
    pieces = [scores[:, BLK * j : BLK * (j + 1)] for j in range(len(oks))]
    pieces = [s if ok is None else jnp.where(ok, s, MASKED) for s, ok in zip(pieces, oks)]
    tallest = functools.reduce(jnp.maximum, pieces)
    tallest = jnp.max(tallest, axis=1, keepdims=True)
    if first:
        peak = jnp.broadcast_to(tallest, (BLK, BLK))
    else:
        before = m_ref[head, rows, :]
        peak = jnp.maximum(before, tallest)
    weights = [jnp.exp2((s - peak) * EXPONENT).astype(jnp.bfloat16) for s in pieces]
    weights = jnp.concatenate(weights, axis=1)
    added = jnp.dot(weights, value_slots, preferred_element_type=jnp.float32)
    if not first:
        rescale = jnp.exp2((before - peak) * EXPONENT)
        rescale = jnp.concatenate([rescale, rescale], axis=1)
        added = acc_ref[head, rows, :] * rescale + added
    acc_ref[head, rows, :] = added
    m_ref[head, rows, :] = peak


def attend_kernel(cfg, width_ref, offset_ref, *refs):
    group, heads, shifts, units, members, begins, ends = cfg
    q_refs, refs = refs[:group], refs[group:]
    held = len(members)
    chunks = [dict(zip(members, refs[held * i : held * (i + 1)])) for i in range(len(shifts))]
    refs = refs[held * len(shifts) :]
    if not begins:
        refs = refs[2:]
    if ends:
        keep_ref, give_ref, m_ref, acc_ref = refs
    else:
        m_ref, acc_ref = refs
    tokens = q_refs[0].shape[0]
    blocks = tokens // BLK
    width = heads * HEAD
    me = lax.axis_index("frame")
    unit, place = me // group, lax.rem(me, group)
    ones = jnp.ones((BLK, HEAD), jnp.bfloat16)

    def pair_slots(b, qf, kf, far, refs):
        distance = jnp.abs(qf - kf)
        present = distance <= RADIUS
        reach = jnp.minimum(distance, RADIUS)
        span = width_ref[qf, reach]
        start = offset_ref[qf, b, reach]
        most = min(MAX_WIDTH[min(far, RADIUS)], blocks)
        found = []
        for j in range(most):
            if most == blocks:
                inside = lax.rem(j - start + blocks, blocks) < span
                if far == 0:
                    inside = inside | ((distance == 0) & (b == j))
                found.append((refs, j, present & inside))
            else:
                inside = None if most == 1 and far * 1 <= RADIUS - 2 * (group - 1) else present & (j < span)
                found.append((refs, lax.rem(start + j, blocks), inside))
        return found

    def gather(found, head, column):
        parts = []
        for ref, block, _ in found:
            if isinstance(block, int):
                at = pl.ds(block * BLK, BLK)
            else:
                at = pl.ds(pl.multiple_of(block * BLK, BLK), BLK)
            parts.append(ref[at, column + head * HEAD : column + (head + 1) * HEAD])
        return parts

    def steps(step, other, chunk, begin):
        far = max(0, step * group - (group - 1))
        most = min(MAX_WIDTH[min(far, RADIUS)], blocks)
        for member in range(group):
            qf = frame_of(unit, place, group, member)
            order = [i for i in (member, *range(group)) if i in members]
            order = list(dict.fromkeys(order))
            batches = [[i] for i in order] if most == blocks else [order]
            for index, batch in enumerate(batches):
                for head in range(heads):
                    for b in range(blocks):
                        found = []
                        for i in batch:
                            kf = frame_of(other, place, group, i)
                            found += pair_slots(b, qf, kf, far, chunk[i])
                        key_slots = jnp.concatenate(gather(found, head, 0), axis=0)
                        value_slots = jnp.concatenate(
                            [
                                jnp.concatenate([v, ones], axis=1)
                                for v in gather(found, head, width)
                            ],
                            axis=0,
                        )
                        rows = slice(member * tokens + b * BLK, member * tokens + (b + 1) * BLK)
                        query = q_refs[member][
                            b * BLK : (b + 1) * BLK, head * HEAD : (head + 1) * HEAD
                        ]
                        oks = [ok for _, _, ok in found]
                        update(
                            rows, query, key_slots, value_slots, oks,
                            m_ref, acc_ref, head, begin and index == 0,
                        )

    facing = 1 - 2 * lax.rem(unit, 2)
    for (step, parity), chunk in zip(shifts, chunks):
        if step == 0:
            steps(0, unit, chunk, begins)
        else:
            other = unit + step * (facing if parity == 0 else -facing)

            @pl.when((other >= 0) & (other < units))
            def _(step=step, other=other, chunk=chunk):
                steps(step, other, chunk, False)

    if ends:
        halves, rank_rows = keep_ref.shape[0] // group, keep_ref.shape[1]
        rank = lax.axis_index("head")
        for head in range(heads):
            columns = slice(head * HEAD, (head + 1) * HEAD)
            for r in range(keep_ref.shape[0]):
                for ref, low in ((keep_ref, 0), (give_ref, 1)):
                    block = rank ^ (2 * (r % halves) + low)
                    start = (r // halves) * tokens + block * rank_rows
                    at = pl.ds(pl.multiple_of(start, rank_rows), rank_rows)
                    both = acc_ref[head, at, :]
                    ref[r, :, columns] = (both[:, :HEAD] / both[:, HEAD:]).astype(ref.dtype)


def attend(cfg, bands, queries, chunks, state):
    group, heads, _, _, _, begins, ends = cfg
    tokens = queries[0].shape[0]
    rows = group * tokens
    m_shape = pltpu.VMEM((heads, rows, BLK), jnp.float32)
    acc_shape = pltpu.VMEM((heads, rows, 2 * HEAD), jnp.float32)
    flat = [in_vmem(c) for pair in chunks for c in pair]
    inputs = [*bands, *[in_vmem(q) for q in queries], *flat, *state]
    outs = [m_shape, acc_shape]
    aliases = {}
    if not begins:
        aliases = {len(inputs) - 2: 0, len(inputs) - 1: 1}
    if ends:
        sent = group * lax.axis_size("head") // 2
        part = pltpu.VMEM((sent, rows // (2 * sent), heads * HEAD), queries[0].dtype)
        outs = [part, part, m_shape, acc_shape]
        aliases = {index: out + 2 for index, out in aliases.items()}
    work = 4 * len(flat) * tokens * rows * heads * HEAD
    return pl.pallas_call(
        functools.partial(attend_kernel, cfg),
        out_shape=outs,
        in_specs=[SMEM] * 2 + [VMEM] * (len(inputs) - 2),
        out_specs=[VMEM] * len(outs),
        input_output_aliases=aliases,
        compiler_params=params(),
        cost_estimate=pl.CostEstimate(flops=work, bytes_accessed=1 << 20, transcendentals=0),
    )(*inputs)


def pack_kernel(keep_ref, got_ref, *outs):
    for r, out in enumerate(outs):
        out[0] = keep_ref[r]
        out[1] = got_ref[r]


def pack(keep, got):
    count, *shape = keep.shape
    return pl.pallas_call(
        pack_kernel,
        out_shape=[pltpu.VMEM((2, *shape), keep.dtype)] * count,
        in_specs=[VMEM] * 2,
        out_specs=[VMEM] * count,
        compiler_params=params(),
        name="pack",
    )(in_vmem(keep), in_vmem(got))


def project_kernel(group, ranks, *refs):
    rows, weights = refs[: group * ranks // 2], refs[group * ranks // 2 : -3]
    out_ref, kept, sem = refs[-3:]
    place = lax.rem(lax.axis_index("frame"), group)
    lefts = []
    for offset in range(ranks):
        parts = [rows[i * ranks // 2 + offset // 2][offset % 2] for i in range(group)]
        left = jnp.concatenate(parts, axis=1)
        if group == 2:
            left = jnp.where(place == 0, left, jnp.concatenate(parts[::-1], axis=1))
        lefts.append(left)
    copies = []
    for part in range(PARTS):
        width = kept.shape[1] // PARTS
        columns = slice(part * width, (part + 1) * width)
        total = None
        for left, weight in zip(lefts, weights):
            term = jnp.dot(left, weight[:, columns], preferred_element_type=jnp.float32)
            total = term if total is None else total + term
        kept[:, columns] = total.astype(kept.dtype)
        copy = pltpu.make_async_copy(kept.at[:, columns], out_ref.at[:, columns], sem.at[part])
        copy.start()
        copies.append(copy)
    for copy in copies:
        copy.wait()


def project(rows, weights, group):
    ranks = len(weights)
    tokens, columns = rows[0].shape[1], weights[0].shape[1]
    return pl.pallas_call(
        functools.partial(project_kernel, group, ranks),
        out_shape=jax.ShapeDtypeStruct((tokens, columns), rows[0].dtype),
        in_specs=[VMEM] * (len(rows) + ranks),
        out_specs=HBM,
        scratch_shapes=[
            pltpu.VMEM((tokens, columns), rows[0].dtype),
            pltpu.SemaphoreType.DMA((PARTS,)),
        ],
        compiler_params=params(),
        cost_estimate=pl.CostEstimate(
            flops=4 * rows[0].size * len(rows) * columns, bytes_accessed=1 << 20, transcendentals=0
        ),
        name="project",
    )(*[in_vmem(r) for r in rows], *[in_vmem(w) for w in weights])


def plan(shape, columns):
    frames, local_heads = shape["frame"], columns // HEAD
    group = 2 if local_heads % 2 == 0 and frames % 2 == 0 else 1
    units = frames // group
    return group, units, min(units - 1, (RADIUS + group - 1) // group)


def edges(units, k, parity):
    sends = []
    for low in range(parity, units - 1, 2):
        if low + 1 - k >= 0:
            sends.append((low, low + 1))
        if low + k < units:
            sends.append((low + 1, low))
    return sends


def on_device(queries, keys, values, band_width, band_offset, out_weight):
    frames, ranks = lax.axis_size("frame"), lax.axis_size("head")
    group, units, furthest = plan({"frame": frames}, queries.shape[1])
    heads = queries.shape[1] // HEAD // group

    def along(value, steps):
        pairs = [(a * group + i, b * group + i) for a, b in steps for i in range(group)]
        return lax.ppermute(value, "frame", pairs)

    bands = (band_width, jnp.transpose(band_offset, (0, 2, 1)))
    *pieces, band_width, band_offset = split(queries, keys, values, bands, group)
    bands = (band_width, band_offset)
    chunks, query_rows = [pieces[0]], [pieces[1]]
    if group == 2:
        swap = [(f, f ^ 1) for f in range(frames)]
        chunks.append(lax.ppermute(pieces[2], "frame", swap))
        query_rows.append(lax.ppermute(pieces[3], "frame", swap))

    weights = {0: out_weight}
    bit = ranks // 2
    while bit:
        for offset in list(weights):
            pairs = [(h, h ^ bit) for h in range(ranks)]
            weights[offset ^ bit] = lax.ppermute(weights[offset], "head", pairs)
        bit //= 2
    weights = [weights[o] for o in range(ranks)]

    held, arrived = [chunks, chunks], []
    for k in range(1, furthest + 1):
        held = [
            [along(c, edges(units, k, parity)) for c in source]
            for parity, source in enumerate(reversed(held))
            if edges(units, k, parity)
        ]
        arrived.append(held)

    everyone = tuple(range(group))
    cfg = (group, heads, ((0, 0),), units, everyone, True, False)
    state = attend(cfg, bands, query_rows, [chunks], [])
    for k, received in enumerate(arrived, 1):
        shifts = tuple((k, parity) for parity in range(2) if edges(units, k, parity))
        last = k == furthest
        for members in [(i,) for i in everyone] if last else [everyone]:
            ends = last and members[-1] == group - 1
            cfg = (group, heads, shifts, units, members, False, ends)
            some = [[chunk[i] for i in members] for chunk in received]
            state = attend(cfg, bands, query_rows, some, state)
    keep, give = state[:2]
    got = lax.ppermute(give, "head", [(h, h ^ 1) for h in range(ranks)])
    packed = pack(keep, got)
    rows = [packed[0]]
    for r in range(1, len(packed)):
        over, high = r // (ranks // 2), 2 * (r % (ranks // 2))
        pairs = [
            (f * ranks + h, (f ^ over) * ranks + (h ^ high))
            for f in range(frames)
            for h in range(ranks)
        ]
        rows.append(lax.ppermute(packed[r], ("frame", "head"), pairs))
    return project(rows, weights, group)


def solution(mesh):
    placed = (P("frame", "head"), P("frame", "head"), P("frame", "head"), P(), P(), P("head", None))
    return jax.shard_map(
        on_device, mesh=mesh, in_specs=placed, out_specs=P(("frame", "head"), None), check_vma=False
    )
```

```python
import functools
import math

import jax
import jax.numpy as jnp
from jax import lax
from jax.experimental import pallas as pl
from jax.experimental.pallas import tpu as pltpu
from jax.sharding import PartitionSpec as P


HEAD = 128
BLK = 128
RADIUS = 7
MAX_WIDTH = (4, 4, 2, 2, 1, 1, 1, 1)
MASKED = -1e30
EXPONENT = math.log2(math.e) / math.sqrt(HEAD)

VMEM = pl.BlockSpec(memory_space=pltpu.VMEM)
SMEM = pl.BlockSpec(memory_space=pltpu.SMEM)
HBM = pl.BlockSpec(memory_space=pltpu.HBM)


def in_vmem(value):
    return pltpu.with_memory_space_constraint(value, pltpu.VMEM)


def in_hbm(value):
    return pltpu.with_memory_space_constraint(value, pltpu.HBM)


def params():
    return pltpu.CompilerParams(vmem_limit_bytes=32 << 20)


def split_kernel(group, q_ref, k_ref, v_ref, width_ref, offset_ref, *refs):
    outs, sem = refs[:-1], refs[-1]
    width = outs[0].shape[1] // 2
    place = lax.rem(lax.axis_index("frame"), group)
    copies = []
    for part in range(group):
        column = (place if part == 0 else 1 - place) * width
        columns = pl.ds(pl.multiple_of(column, HEAD), width)
        pair, rows = outs[2 * part], outs[2 * part + 1]
        for source, target in (
            (k_ref, pair.at[:, :width]),
            (v_ref, pair.at[:, width:]),
            (q_ref, rows),
        ):
            copies.append(
                pltpu.make_async_copy(source.at[:, columns], target, sem.at[len(copies)])
            )
    for source, target in ((width_ref, outs[-2]), (offset_ref, outs[-1])):
        copies.append(pltpu.make_async_copy(source, target, sem.at[len(copies)]))
    for copy in copies:
        copy.start()
    for copy in copies:
        copy.wait()


def split(queries, keys, values, bands, group):
    tokens, columns = queries.shape
    width = columns // group
    pair = pltpu.VMEM((tokens, 2 * width), queries.dtype)
    rows = pltpu.VMEM((tokens, width), queries.dtype)
    return pl.pallas_call(
        functools.partial(split_kernel, group),
        out_shape=[pair, rows] * group + [pltpu.SMEM(b.shape, b.dtype) for b in bands],
        in_specs=[HBM] * 5,
        out_specs=[VMEM] * (2 * group) + [SMEM] * 2,
        scratch_shapes=[pltpu.SemaphoreType.DMA((3 * group + 2,))],
        compiler_params=params(),
        name="split",
    )(*[in_hbm(v) for v in (queries, keys, values, *bands)])


def frame_of(unit, place, group, member):
    return unit * group + (place if member == 0 else group - 1 - place)


def update(rows, query, key_slots, value_slots, oks, m_ref, acc_ref, head, first):
    scores = lax.dot_general(
        query, key_slots, (((1,), (1,)), ((), ())), preferred_element_type=jnp.float32
    )
    pieces = [scores[:, BLK * j : BLK * (j + 1)] for j in range(len(oks))]
    pieces = [s if ok is None else jnp.where(ok, s, MASKED) for s, ok in zip(pieces, oks)]
    tallest = functools.reduce(jnp.maximum, pieces)
    tallest = jnp.max(tallest, axis=1, keepdims=True)
    if first:
        peak = jnp.broadcast_to(tallest, (BLK, BLK))
    else:
        before = m_ref[head, rows, :]
        peak = jnp.maximum(before, tallest)
    weights = [jnp.exp2((s - peak) * EXPONENT).astype(jnp.bfloat16) for s in pieces]
    weights = jnp.concatenate(weights, axis=1)
    added = jnp.dot(weights, value_slots, preferred_element_type=jnp.float32)
    if not first:
        rescale = jnp.exp2((before - peak) * EXPONENT)
        rescale = jnp.concatenate([rescale, rescale], axis=1)
        added = acc_ref[head, rows, :] * rescale + added
    acc_ref[head, rows, :] = added
    m_ref[head, rows, :] = peak


def attend_kernel(cfg, width_ref, offset_ref, *refs):
    group, heads, shifts, units, begins, ends = cfg
    q_refs, refs = refs[:group], refs[group:]
    chunks = [refs[group * i : group * (i + 1)] for i in range(len(shifts))]
    refs = refs[group * len(shifts) :]
    if not begins:
        refs = refs[2:]
    if ends:
        keep_ref, first_ref, give_ref, m_ref, acc_ref = refs
    else:
        m_ref, acc_ref = refs
    tokens = q_refs[0].shape[0]
    blocks = tokens // BLK
    width = heads * HEAD
    me = lax.axis_index("frame")
    unit, place = me // group, lax.rem(me, group)
    ones = jnp.ones((BLK, HEAD), jnp.bfloat16)

    def pair_slots(b, qf, kf, far, refs):
        distance = jnp.abs(qf - kf)
        present = distance <= RADIUS
        reach = jnp.minimum(distance, RADIUS)
        span = width_ref[qf, reach]
        start = offset_ref[qf, b, reach]
        most = min(MAX_WIDTH[min(far, RADIUS)], blocks)
        found = []
        for j in range(most):
            if most == blocks:
                inside = lax.rem(j - start + blocks, blocks) < span
                if far == 0:
                    inside = inside | ((distance == 0) & (b == j))
                found.append((refs, j, present & inside))
            else:
                inside = None if most == 1 and far * 1 <= RADIUS - 2 * (group - 1) else present & (j < span)
                found.append((refs, lax.rem(start + j, blocks), inside))
        return found

    def gather(found, head, column):
        parts = []
        for ref, block, _ in found:
            if isinstance(block, int):
                at = pl.ds(block * BLK, BLK)
            else:
                at = pl.ds(pl.multiple_of(block * BLK, BLK), BLK)
            parts.append(ref[at, column + head * HEAD : column + (head + 1) * HEAD])
        return parts

    def steps(step, other, chunk, begin):
        far = max(0, step * group - (group - 1))
        most = min(MAX_WIDTH[min(far, RADIUS)], blocks)
        for member in range(group):
            qf = frame_of(unit, place, group, member)
            order = [member] + [i for i in range(group) if i != member]
            batches = [[i] for i in order] if most == blocks else [order]
            for index, batch in enumerate(batches):
                for head in range(heads):
                    for b in range(blocks):
                        found = []
                        for i in batch:
                            kf = frame_of(other, place, group, i)
                            found += pair_slots(b, qf, kf, far, chunk[i])
                        key_slots = jnp.concatenate(gather(found, head, 0), axis=0)
                        value_slots = jnp.concatenate(
                            [
                                jnp.concatenate([v, ones], axis=1)
                                for v in gather(found, head, width)
                            ],
                            axis=0,
                        )
                        rows = slice(member * tokens + b * BLK, member * tokens + (b + 1) * BLK)
                        query = q_refs[member][
                            b * BLK : (b + 1) * BLK, head * HEAD : (head + 1) * HEAD
                        ]
                        oks = [ok for _, _, ok in found]
                        update(
                            rows, query, key_slots, value_slots, oks,
                            m_ref, acc_ref, head, begin and index == 0,
                        )

    facing = 1 - 2 * lax.rem(unit, 2)
    for (step, parity), chunk in zip(shifts, chunks):
        if step == 0:
            steps(0, unit, chunk, begins)
        else:
            other = unit + step * (facing if parity == 0 else -facing)

            @pl.when((other >= 0) & (other < units))
            def _(step=step, other=other, chunk=chunk):
                steps(step, other, chunk, False)

    if ends:
        sent, rank_rows = give_ref.shape[0], give_ref.shape[1]
        halves = sent // group
        rank = lax.axis_index("head")
        for head in range(heads):
            columns = slice(head * HEAD, (head + 1) * HEAD)
            for r in range(sent):
                for low in range(2):
                    ref, slot = (give_ref, r) if low else (keep_ref, r)
                    if low == 0 and r == sent - 1:
                        ref, slot = first_ref, 0
                    block = rank ^ (2 * (r % halves) + low)
                    start = (r // halves) * tokens + block * rank_rows
                    at = pl.ds(pl.multiple_of(start, rank_rows), rank_rows)
                    both = acc_ref[head, at, :]
                    ref[slot, :, columns] = (both[:, :HEAD] / both[:, HEAD:]).astype(ref.dtype)


def attend(cfg, bands, queries, chunks, state):
    group, heads, _, _, begins, ends = cfg
    tokens = queries[0].shape[0]
    rows = group * tokens
    m_shape = pltpu.VMEM((heads, rows, BLK), jnp.float32)
    acc_shape = pltpu.VMEM((heads, rows, 2 * HEAD), jnp.float32)
    flat = [in_vmem(c) for pair in chunks for c in pair]
    inputs = [*bands, *[in_vmem(q) for q in queries], *flat, *state]
    outs = [m_shape, acc_shape]
    aliases = {}
    if not begins:
        aliases = {len(inputs) - 2: 0, len(inputs) - 1: 1}
    if ends:
        sent = group * lax.axis_size("head") // 2
        parts = [
            pltpu.VMEM((count, rows // (2 * sent), heads * HEAD), queries[0].dtype)
            for count in (sent - 1, 1, sent)
        ]
        outs = [*parts, m_shape, acc_shape]
        aliases = {index: out + 3 for index, out in aliases.items()}
    work = 4 * len(flat) * tokens * rows * heads * HEAD
    return pl.pallas_call(
        functools.partial(attend_kernel, cfg),
        out_shape=outs,
        in_specs=[SMEM] * 2 + [VMEM] * (len(inputs) - 2),
        out_specs=[VMEM] * len(outs),
        input_output_aliases=aliases,
        compiler_params=params(),
        cost_estimate=pl.CostEstimate(flops=work, bytes_accessed=1 << 20, transcendentals=0),
    )(*inputs)


def pack_kernel(keep_ref, got_ref, *outs):
    *pairs, alone = outs
    for r, out in enumerate(pairs):
        out[0] = keep_ref[r]
        out[1] = got_ref[r]
    alone[0] = got_ref[len(pairs)]


def pack(keep, got):
    count, *shape = keep.shape
    return pl.pallas_call(
        pack_kernel,
        out_shape=[pltpu.VMEM((2, *shape), keep.dtype)] * count
        + [pltpu.VMEM((1, *shape), keep.dtype)],
        in_specs=[VMEM] * 2,
        out_specs=[VMEM] * (count + 1),
        compiler_params=params(),
        name="pack",
    )(in_vmem(keep), in_vmem(got))


def project_kernel(group, ranks, *refs):
    sent = group * ranks // 2
    rows, weights, out_ref = refs[: sent + 1], refs[sent + 1 : -1], refs[-1]
    place = lax.rem(lax.axis_index("frame"), group)
    total = None
    for offset, weight in enumerate(weights):
        parts = []
        for i in range(group):
            r = i * ranks // 2 + offset // 2
            apart = r == sent - 1
            parts.append(rows[r + offset % 2][0] if apart else rows[r][offset % 2])
        left = jnp.concatenate(parts, axis=1)
        if group == 2:
            left = jnp.where(place == 0, left, jnp.concatenate(parts[::-1], axis=1))
        term = jnp.dot(left, weight[...], preferred_element_type=jnp.float32)
        total = term if total is None else total + term
    out_ref[...] = total.astype(out_ref.dtype)


def project(rows, weights, group):
    ranks = len(weights)
    tokens, columns = rows[0].shape[1], weights[0].shape[1]
    return pl.pallas_call(
        functools.partial(project_kernel, group, ranks),
        out_shape=jax.ShapeDtypeStruct((tokens, columns), rows[0].dtype),
        in_specs=[VMEM] * (len(rows) + ranks),
        out_specs=VMEM,
        compiler_params=params(),
        cost_estimate=pl.CostEstimate(
            flops=4 * rows[0].size * (len(rows) - 1) * columns, bytes_accessed=1 << 20, transcendentals=0
        ),
        name="project",
    )(*[in_vmem(r) for r in rows], *[in_vmem(w) for w in weights])


def plan(shape, columns):
    frames, local_heads = shape["frame"], columns // HEAD
    group = 2 if local_heads % 2 == 0 and frames % 2 == 0 else 1
    units = frames // group
    return group, units, min(units - 1, (RADIUS + group - 1) // group)


def edges(units, k, parity):
    sends = []
    for low in range(parity, units - 1, 2):
        if low + 1 - k >= 0:
            sends.append((low, low + 1))
        if low + k < units:
            sends.append((low + 1, low))
    return sends


def on_device(queries, keys, values, band_width, band_offset, out_weight):
    frames, ranks = lax.axis_size("frame"), lax.axis_size("head")
    group, units, furthest = plan({"frame": frames}, queries.shape[1])
    heads = queries.shape[1] // HEAD // group

    def along(value, steps):
        pairs = [(a * group + i, b * group + i) for a, b in steps for i in range(group)]
        return lax.ppermute(value, "frame", pairs)

    bands = (band_width, jnp.transpose(band_offset, (0, 2, 1)))
    *pieces, band_width, band_offset = split(queries, keys, values, bands, group)
    bands = (band_width, band_offset)
    chunks, query_rows = [pieces[0]], [pieces[1]]
    if group == 2:
        swap = [(f, f ^ 1) for f in range(frames)]
        chunks.append(lax.ppermute(pieces[2], "frame", swap))
        query_rows.append(lax.ppermute(pieces[3], "frame", swap))

    weights = {0: out_weight}
    bit = ranks // 2
    while bit:
        for offset in list(weights):
            pairs = [(h, h ^ bit) for h in range(ranks)]
            weights[offset ^ bit] = lax.ppermute(weights[offset], "head", pairs)
        bit //= 2
    weights = [weights[o] for o in range(ranks)]

    held, arrived = [chunks, chunks], []
    for k in range(1, furthest + 1):
        held = [
            [along(c, edges(units, k, parity)) for c in source]
            for parity, source in enumerate(reversed(held))
            if edges(units, k, parity)
        ]
        arrived.append(held)

    cfg = (group, heads, ((0, 0),), units, True, False)
    state = attend(cfg, bands, query_rows, [chunks], [])
    for k, received in enumerate(arrived, 1):
        shifts = tuple((k, parity) for parity in range(2) if edges(units, k, parity))
        cfg = (group, heads, shifts, units, False, k == furthest)
        state = attend(cfg, bands, query_rows, received, state)

    def across(value, r):
        over, high = r // (ranks // 2), 2 * (r % (ranks // 2))
        pairs = [
            (f * ranks + h, (f ^ over) * ranks + (h ^ high))
            for f in range(frames)
            for h in range(ranks)
        ]
        return lax.ppermute(value, ("frame", "head"), pairs)

    keep, first, give = state[:3]
    got = lax.ppermute(give, "head", [(h, h ^ 1) for h in range(ranks)])
    count = keep.shape[0]
    first = across(first, count)
    packed = pack(keep, got)
    rows = [packed[0], *[across(packed[r], r) for r in range(1, count)]]
    rows += [first, across(packed[count], count)]
    return project(rows, weights, group)


def solution(mesh):
    placed = (P("frame", "head"), P("frame", "head"), P("frame", "head"), P(), P(), P("head", None))
    return jax.shard_map(
        on_device, mesh=mesh, in_specs=placed, out_specs=P(("frame", "head"), None), check_vma=False
    )
```
